16 devices in a mesh: dp: 4 (over z, y), ep: 4 (over x, core).
Axes of the slice: x: 2, y: 2, z: 2, core: 2. Of those that a mesh axis runs over, the one named last changes fastest.
Arguments:
- tokens: bfloat16 [4096, 2048], P(('dp', 'ep')), parts along dimension 0
- expert_ids: int32 [4096, 6], P(('dp', 'ep')), parts along dimension 0
- gate_vals: float32 [4096, 6], P(('dp', 'ep')), parts along dimension 0
- slots: int32 [4096, 6], P(('dp', 'ep')), parts along dimension 0
- shared_w1: bfloat16 [2048, 2816], replicated
- shared_w3: bfloat16 [2048, 2816], replicated
- shared_w2: bfloat16 [2816, 2048], replicated
- shared_gate: bfloat16 [2048], replicated
- expert_w1: bfloat16 [64, 2048, 1408], P('ep')
- expert_w3: bfloat16 [64, 2048, 1408], P('ep')
- expert_w2: bfloat16 [64, 1408, 2048], P('ep')
Outputs:
- output: bfloat16 [4096, 2048], P(('dp', 'ep')), parts along dimension 0
There are 4 independent parts. The reference program is written for one: setup_inputs(seed, part) draws one part's arguments, and reference() takes and returns one part's arrays. A program takes and returns all parts, laid end to end along the dimension named above; an argument that names none is the same for every part.
All inputs are finite; a program needn't handle non-finite values.
Results may differ from the reference program's by a relative error of at most 0.00518169.
Values are sent between devices in bfloat16 or wider.
A program may use at most 1.25 GiB of HBM per device.

```python
import jax
import jax.numpy as jnp
from jax import lax

EP_SIZE = 4
TOKENS_DEV = 256
HIDDEN = 2048
EXPERTS = 64
TOP_K = 6
EXPERT_FF = 1408
SHARED_FF = 2816
CAPACITY = 48

NUM_TOKENS = EP_SIZE * TOKENS_DEV
BUF_ROWS = EXPERTS * CAPACITY


def draw_routes(route_key):
    score_key, bias_key, hot_key = jax.random.split(route_key, 3)
    scores = jax.random.randint(score_key, (NUM_TOKENS, EXPERTS), 0, 4096)
    expert_bias = jax.random.randint(bias_key, (EXPERTS,), 0, 1024)
    hot_expert = jax.random.randint(hot_key, (), 0, EXPERTS)
    expert_pos = jnp.arange(EXPERTS)
    forced = ((jnp.arange(NUM_TOKENS) % 2) == 0)[:, None] & (expert_pos[None, :] == hot_expert)
    total_score = scores + expert_bias[None, :] + jnp.where(forced, 8192, 0)
    distinct = total_score * EXPERTS + expert_pos[None, :]
    return lax.top_k(distinct, TOP_K)[1].astype(jnp.int32)


def source_slots(src_ids):
    flat_ids = src_ids.reshape(TOKENS_DEV * TOP_K)
    one_hot = (flat_ids[:, None] == jnp.arange(EXPERTS)[None, :]).astype(jnp.int32)
    earlier = jnp.cumsum(one_hot, axis=0) - one_hot
    position = jnp.sum(earlier * one_hot, axis=1)
    return jnp.where(position < CAPACITY, position, -1).reshape(TOKENS_DEV, TOP_K).astype(jnp.int32)


def normal_stack(stack_key, rows, cols):
    def one_matrix(one_key):
        return (jax.random.normal(one_key, (rows, cols), jnp.float32) * rows ** -0.5).astype(jnp.bfloat16)
    return lax.map(one_matrix, jax.random.split(stack_key, EXPERTS))


def setup_inputs(seed: int = 0, part: int = 0) -> dict:
    part_key = jax.random.fold_in(jax.random.key(seed), part)
    tok_key, route_key, gate_key = jax.random.split(part_key, 3)
    weight_keys = jax.random.split(jax.random.key(seed + 1), 7)
    tokens = jax.random.normal(tok_key, (NUM_TOKENS, HIDDEN), jnp.float32).astype(jnp.bfloat16)
    expert_ids = draw_routes(route_key)
    slots = lax.map(source_slots, expert_ids.reshape(EP_SIZE, TOKENS_DEV, TOP_K)).reshape(NUM_TOKENS, TOP_K)
    gate_vals = jax.random.uniform(gate_key, (NUM_TOKENS, TOP_K), jnp.float32, 0.5, 1.5) * TOP_K ** -0.5
    shared_w1 = (jax.random.normal(weight_keys[0], (HIDDEN, SHARED_FF), jnp.float32) * HIDDEN ** -0.5).astype(jnp.bfloat16)
    shared_w3 = (jax.random.normal(weight_keys[1], (HIDDEN, SHARED_FF), jnp.float32) * HIDDEN ** -0.5).astype(jnp.bfloat16)
    shared_w2 = (jax.random.normal(weight_keys[2], (SHARED_FF, HIDDEN), jnp.float32) * SHARED_FF ** -0.5).astype(jnp.bfloat16)
    shared_gate = (jax.random.normal(weight_keys[3], (HIDDEN,), jnp.float32) * 2.0 * HIDDEN ** -0.5).astype(jnp.bfloat16)
    expert_w1 = normal_stack(weight_keys[4], HIDDEN, EXPERT_FF)
    expert_w3 = normal_stack(weight_keys[5], HIDDEN, EXPERT_FF)
    expert_w2 = normal_stack(weight_keys[6], EXPERT_FF, HIDDEN)
    return {'tokens': tokens, 'expert_ids': expert_ids, 'gate_vals': gate_vals, 'slots': slots, 'shared_w1': shared_w1, 'shared_w3': shared_w3, 'shared_w2': shared_w2, 'shared_gate': shared_gate, 'expert_w1': expert_w1, 'expert_w3': expert_w3, 'expert_w2': expert_w2}


def swiglu_rows(rows, w_up, w_in, w_down):
    act_a = jnp.dot(rows, w_up, preferred_element_type=jnp.float32)
    act_b = jnp.dot(rows, w_in, preferred_element_type=jnp.float32)
    hidden_act = (jax.nn.silu(act_a) * act_b).astype(jnp.bfloat16)
    return jnp.dot(hidden_act, w_down, preferred_element_type=jnp.float32)


def reference(tokens, expert_ids, gate_vals, slots, shared_w1, shared_w3, shared_w2, shared_gate, expert_w1, expert_w3, expert_w2):
    src_tokens = tokens.reshape(EP_SIZE, TOKENS_DEV, HIDDEN)
    kept_mask = slots >= 0
    slot_dest = jnp.where(kept_mask, expert_ids * CAPACITY + slots, BUF_ROWS)
    flat_dest = slot_dest.reshape(EP_SIZE, TOKENS_DEV * TOP_K)
    copy_tok = jnp.arange(TOKENS_DEV * TOP_K, dtype=jnp.int32) // TOP_K

    def dispatch_one(operands):
        src_rows, src_dest = operands
        row_owner = jnp.full((BUF_ROWS + 1,), TOKENS_DEV, jnp.int32).at[src_dest].set(copy_tok)
        return jnp.take(src_rows, row_owner[:BUF_ROWS], axis=0, mode='fill', fill_value=0)

    buffers = lax.map(dispatch_one, (src_tokens, flat_dest))
    per_expert = buffers.reshape(EP_SIZE, EXPERTS, CAPACITY, HIDDEN).transpose(1, 0, 2, 3).reshape(EXPERTS, EP_SIZE * CAPACITY, HIDDEN)

    def expert_one(operands):
        rows, w_up, w_in, w_down = operands
        return swiglu_rows(rows, w_up, w_in, w_down).astype(jnp.bfloat16)

    expert_out = lax.map(expert_one, (per_expert, expert_w1, expert_w3, expert_w2))
    returned = expert_out.reshape(EXPERTS, EP_SIZE, CAPACITY, HIDDEN).transpose(1, 0, 2, 3).reshape(EP_SIZE, BUF_ROWS, HIDDEN)
    weights = jnp.where(kept_mask, gate_vals, 0.0).reshape(EP_SIZE, TOKENS_DEV, TOP_K)
    src_dest = slot_dest.reshape(EP_SIZE, TOKENS_DEV, TOP_K)

    def combine_one(operands):
        src_rows, src_out, src_idx, src_weights = operands
        picked = jnp.take(src_out, src_idx, axis=0, mode='fill', fill_value=0)
        routed = jnp.einsum('tk,tkd->td', src_weights, picked.astype(jnp.float32))
        gate_logit = jnp.dot(src_rows, shared_gate, preferred_element_type=jnp.float32)
        shared_out = jax.nn.sigmoid(gate_logit)[:, None] * swiglu_rows(src_rows, shared_w1, shared_w3, shared_w2)
        return (src_rows.astype(jnp.float32) + shared_out + routed).astype(jnp.bfloat16)

    result = lax.map(combine_one, (src_tokens, returned, src_dest, weights))
    return result.reshape(NUM_TOKENS, HIDDEN)
```

```python
import functools

import jax
import jax.numpy as jnp
from jax import lax
from jax.experimental import pallas as pl
from jax.experimental.pallas import tpu as pltpu
from jax.sharding import PartitionSpec as P

MESH = pl.DeviceIdType.MESH
F32 = jnp.float32
BF16 = jnp.bfloat16
CHUNK = 256
RING = 5
PIECES = 4
GROUP = 4
LAG = 2
BF16_MAX = 3.3895313892515355e38


def moe_kernel(cfg, tok, route, sgate, sw1, sw3, sw2, ew1, ew3, ew2, y,
               toks, rts, wbuf, xg, h, hs, gs, rbuf, sig, acc, send3, send1, recv3, recv1, recvu,
               load_sem, wsem, tsem, tok_send, tok_recv, rt_send, rt_recv,
               s3_send, s1_send, su_send, r3_sem, r1_sem, ru_sem):
    n_tok, hidden, n_exp, ff, cap, top_k = cfg
    rows = 4 * cap
    n_chunks = hidden // CHUNK
    per_slot = ff // CHUNK
    n_sub = RING * per_slot
    n_items = 2 * (n_exp + 2)
    per_chunk = n_exp + 2
    n_tiles = n_chunks * per_chunk
    piece = n_tok // PIECES
    slots_all = n_exp * cap

    dp = lax.axis_index('dp')
    me = lax.axis_index('ep')
    partner = (dp, me + 1 - 2 * lax.rem(me, 2))
    across = (dp, lax.rem(me + 2, 4))
    diagonal = (dp, 3 - me)

    def item_copy(item, slot):
        def desc(src):
            return pltpu.make_async_copy(src, wbuf.at[slot], wsem.at[slot])
        return desc

    def shared_item(item):
        src = (sw1, sw3)[item % 2].at[:, pl.ds((item // 2) * ff, ff)]
        return pltpu.make_async_copy(src, wbuf.at[item % RING], wsem.at[item % RING])

    def expert_item(exp, which):
        slot = lax.rem(2 * exp + 4 + which, RING)
        return pltpu.make_async_copy((ew1, ew3)[which].at[exp], wbuf.at[slot], wsem.at[slot])

    def tile_dst(tile):
        sub = lax.rem(tile, n_sub)
        slot = lax.rem(1 + sub // per_slot, RING)
        lane = pl.multiple_of(lax.rem(sub, per_slot) * CHUNK, CHUNK)
        return slot, lane, sub

    def tile_view(tile):
        slot, lane, sub = tile_dst(tile)
        return wbuf.at[slot, pl.ds(0, ff), pl.ds(lane, CHUNK)], tsem.at[sub]

    def start_tile(tile):
        chunk, idx = tile // per_chunk, lax.rem(tile, per_chunk)
        col = pl.ds(pl.multiple_of(chunk * CHUNK, CHUNK), CHUNK)
        dst, sem = tile_view(tile)

        @pl.when(idx < n_exp)
        def _():
            pltpu.make_async_copy(ew2.at[idx, :, col], dst, sem).start()

        @pl.when(idx >= n_exp)
        def _():
            row = pl.multiple_of((idx - n_exp) * ff, 128)
            pltpu.make_async_copy(sw2.at[pl.ds(row, ff), col], dst, sem).start()

    def wait_tile(tile):
        dst, sem = tile_view(tile)
        pltpu.make_async_copy(ew2.at[0, :, pl.ds(0, CHUNK)], dst, sem).wait()

    def load_tile(tile):
        slot, lane, _ = tile_dst(tile)
        return wbuf[slot, pl.ds(0, ff), pl.ds(lane, CHUNK)]

    own_load = pltpu.make_async_copy(tok, toks.at[0], load_sem)
    own_load.start()
    for item in range(4):
        shared_item(item).start()
    expert_item(0, 0).start()

    barrier = pltpu.get_barrier_semaphore()
    for peer in (partner, across, diagonal):
        pl.semaphore_signal(barrier, inc=1, device_id=peer, device_id_type=MESH)
    pl.semaphore_wait(barrier, 3)
    own_load.wait()

    def remote(src, dst, send, recv, peer):
        return pltpu.make_async_remote_copy(src_ref=src, dst_ref=dst, send_sem=send, recv_sem=recv,
                                            device_id=peer, device_id_type=MESH)

    def piece_of(ref, i):
        return ref.at[pl.ds(i * piece, piece)]

    rt_copies = [remote(route, rts.at[d], rt_send.at[d], rt_recv.at[d], peer)
                 for d, peer in ((1, partner), (2, across), (3, diagonal))]
    for copy in rt_copies:
        copy.start()
    tok_across = [remote(piece_of(toks.at[0], i), piece_of(toks.at[2], i), tok_send.at[i], tok_recv.at[i], across)
                  for i in range(PIECES)]
    for copy in tok_across:
        copy.start()
    tok_partner = remote(toks.at[0], toks.at[1], tok_send.at[2 * PIECES], tok_recv.at[2 * PIECES], partner)
    tok_partner.start()
    tok_relay = [remote(piece_of(toks.at[2], i), piece_of(toks.at[3], i), tok_send.at[PIECES + i],
                        tok_recv.at[PIECES + i], partner) for i in range(PIECES)]

    def swiglu_cols(x, slot1, slot3, store):
        def block(i, carry):
            col = pl.multiple_of(i * CHUNK, CHUNK)
            a = jnp.dot(x(), wbuf[slot1, :, pl.ds(col, CHUNK)], preferred_element_type=F32)
            b = jnp.dot(x(), wbuf[slot3, :, pl.ds(col, CHUNK)], preferred_element_type=F32)
            store(col, CHUNK, (jax.nn.silu(a) * b).astype(BF16))
            return carry
        lax.fori_loop(0, per_slot, block, 0)
        done = per_slot * CHUNK
        rest = ff - done
        w = jnp.concatenate([wbuf[slot1, :, pl.ds(done, rest)], wbuf[slot3, :, pl.ds(done, rest)]], axis=1)
        ab = jnp.dot(x(), w, preferred_element_type=F32)
        store(done, rest, (jax.nn.silu(ab[:, :rest]) * ab[:, rest:]).astype(BF16))

    for half in range(2):
        shared_item(2 * half).wait()
        shared_item(2 * half + 1).wait()

        def store_shared(col, width, value):
            hs[half, :, pl.ds(col, width)] = value

        swiglu_cols(lambda: toks[0], (2 * half) % RING, (2 * half + 1) % RING, store_shared)
        expert_item(half, 1).start()
        expert_item(half + 1, 0).start()

    logit = jnp.sum(toks[0].astype(F32) * sgate[...].astype(F32), axis=1, keepdims=True)
    sig[...] = jnp.broadcast_to(jax.nn.sigmoid(logit), sig.shape)

    for copy in rt_copies:
        copy.wait_recv()
    tok_partner.wait_recv()
    base = (me * slots_all).astype(F32)

    def route_rows(d):
        return route if d == 0 else rts.at[d]

    for d in range(4):
        def weight_block(i, carry):
            row = (lax.broadcasted_iota(jnp.int32, (128, n_tok), 0) + i * 128).astype(F32) + base
            g = jnp.zeros((128, n_tok), F32)
            for k in range(top_k):
                g += jnp.where(row == route_rows(d)[k:k + 1, :], route_rows(d)[8 + k:9 + k, :], 0.0)
            g = g.T
            g1 = jnp.minimum(g, BF16_MAX).astype(BF16)
            left = g - g1.astype(F32)
            g2 = left.astype(BF16)
            g3 = (left - g2.astype(F32)).astype(BF16)
            for part, value in enumerate((g1, g2, g3)):
                gs[d, :, pl.ds(pl.multiple_of(part * slots_all + i * 128, 128), 128)] = value
            return carry
        lax.fori_loop(0, slots_all // 128, weight_block, 0)

    for arrived, relay in zip(tok_across, tok_relay):
        arrived.wait_recv()
        relay.start()
    for relay in tok_relay:
        relay.wait_recv()

    def group_step(g, carry):
        for d in range(4):
            row = (lax.broadcasted_iota(jnp.int32, (GROUP * cap, n_tok), 0) + g * (GROUP * cap)).astype(F32) + base
            pick = jnp.zeros((GROUP * cap, n_tok), F32)
            for k in range(top_k):
                pick += jnp.where(row == route_rows(d)[k:k + 1, :], 1.0, 0.0)
            pick = pick.astype(BF16)

            def gather_cols(i, carry):
                col = pl.ds(pl.multiple_of(i * 512, 512), 512)
                got = jnp.dot(pick, toks[d, :, col], preferred_element_type=F32).astype(BF16)
                for e in range(GROUP):
                    xg[e, pl.ds(d * cap, cap), col] = got[e * cap:(e + 1) * cap]
                return carry
            lax.fori_loop(0, hidden // 512, gather_cols, 0)

        def expert_step(i, carry):
            exp = g * GROUP + i
            expert_item(exp, 0).wait()
            expert_item(exp, 1).wait()

            def store_h(col, width, value):
                h[exp, :, pl.ds(col, width)] = value

            slot1, slot3 = lax.rem(2 * exp + 4, RING), lax.rem(2 * exp + 5, RING)
            swiglu_cols(lambda: xg[i], slot1, slot3, store_h)

            @pl.when(exp + 2 < n_exp)
            def _():
                expert_item(exp + 2, 1).start()

            @pl.when(exp + 3 < n_exp)
            def _():
                expert_item(exp + 3, 0).start()

            @pl.when(exp == n_exp - 3)
            def _():
                for t in range(per_slot):
                    start_tile(jnp.int32(t))

            @pl.when(exp == n_exp - 2)
            def _():
                for t in range(per_slot, 3 * per_slot):
                    start_tile(jnp.int32(t))

            @pl.when(exp == n_exp - 1)
            def _():
                for t in range(3 * per_slot, 5 * per_slot):
                    start_tile(jnp.int32(t))
            return carry
        lax.fori_loop(0, GROUP, expert_step, 0)
        return carry
    lax.fori_loop(0, n_exp // GROUP, group_step, 0)

    def next_tile(tile):
        @pl.when(tile + n_sub < n_tiles)
        def _():
            start_tile(tile + n_sub)

    def combine(d):
        r = rbuf[d]
        return jnp.dot(gs[d], jnp.concatenate([r, r, r], axis=0), preferred_element_type=F32)

    def to_partner3(j):
        return remote(send3.at[lax.rem(j, 2)], recv3.at[j], s3_send.at[lax.rem(j, 2)], r3_sem.at[j], partner)

    def to_partner1(j):
        return remote(send1.at[lax.rem(j, 2)], recv1.at[j], s1_send.at[lax.rem(j, 2)], r1_sem.at[j], partner)

    def to_across(j):
        return remote(recv3.at[j], recvu.at[j], su_send.at[j], ru_sem.at[j], across)

    def finish(j):
        to_partner1(j).wait_recv()
        to_across(j).wait_recv()
        col = pl.ds(pl.multiple_of(j * CHUNK, CHUNK), CHUNK)
        y[:, col] = (acc[j] + recv1[j] + recvu[j]).astype(y.dtype)

    def chunk_step(j, carry):
        first = j * per_chunk

        def pair_step(i, carry):
            tile = first + 2 * i
            wait_tile(tile)
            wait_tile(tile + 1)
            for u in range(2):
                exp = 2 * i + u
                r = jnp.dot(h[exp], load_tile(tile + u), preferred_element_type=F32).astype(BF16)
                for d in range(4):
                    rbuf[d, pl.ds(pl.multiple_of(exp * cap, 16), cap), :] = r[d * cap:(d + 1) * cap]
            next_tile(tile)
            next_tile(tile + 1)
            return carry
        lax.fori_loop(0, n_exp // 2, pair_step, 0)

        @pl.when(j >= 2)
        def _():
            to_partner3(j - 2).wait_send()
            to_partner1(j - 2).wait_send()
        send3[lax.rem(j, 2)] = combine(3)
        to_partner3(j).start()
        send1[lax.rem(j, 2)] = combine(1)
        to_partner1(j).start()
        part2 = combine(2)
        to_partner3(j).wait_recv()
        recv3[j] = recv3[j] + part2
        to_across(j).start()

        tile = first + n_exp
        wait_tile(tile)
        wait_tile(tile + 1)
        s = (jnp.dot(hs[0], load_tile(tile), preferred_element_type=F32)
             + jnp.dot(hs[1], load_tile(tile + 1), preferred_element_type=F32))
        next_tile(tile)
        next_tile(tile + 1)
        col = pl.ds(pl.multiple_of(j * CHUNK, CHUNK), CHUNK)
        acc[j] = toks[0, :, col].astype(F32) + sig[:, 0:1] * s + combine(0)

        @pl.when(j >= LAG)
        def _():
            finish(j - LAG)
        return carry
    lax.fori_loop(0, n_chunks, chunk_step, 0)

    def last_step(j, carry):
        finish(j)
        return carry
    lax.fori_loop(n_chunks - LAG, n_chunks, last_step, 0)

    for copy in rt_copies + tok_across + tok_relay + [tok_partner]:
        copy.wait_send()
    for j in range(n_chunks - 2, n_chunks):
        to_partner3(j).wait_send()
        to_partner1(j).wait_send()

    def drain(j, carry):
        to_across(j).wait_send()
        return carry
    lax.fori_loop(0, n_chunks, drain, 0)


def solution(mesh):
    num_ep = mesh.shape['ep']
    row_spec = P(('dp', 'ep'), None)
    expert_spec = P('ep', None, None)

    def device_step(tokens, expert_ids, gate_vals, slots, shared_w1, shared_w3, shared_w2, shared_gate, expert_w1, expert_w3, expert_w2):
        n_tok, hidden = tokens.shape
        top_k = expert_ids.shape[1]
        n_exp, _, ff = expert_w1.shape
        num_experts = n_exp * num_ep
        cap = 8 * ((2 * n_tok * top_k + 8 * num_experts - 1) // (8 * num_experts))
        rows = num_ep * cap
        n_chunks = hidden // CHUNK
        per_slot = ff // CHUNK

        dest = jnp.where(slots >= 0, expert_ids * cap + slots, -1).astype(F32)
        pad = ((0, 8 - top_k), (0, 0))
        route = jnp.concatenate([jnp.pad(dest.T, pad, constant_values=-1.0), jnp.pad(gate_vals.T, pad)], axis=0)

        anywhere = pl.BlockSpec(memory_space=pl.ANY)
        vmem = pl.BlockSpec(memory_space=pltpu.VMEM)
        dma = pltpu.SemaphoreType.DMA
        block = (n_tok, CHUNK)
        return pl.pallas_call(
            functools.partial(moe_kernel, (n_tok, hidden, n_exp, ff, cap, top_k)),
            out_shape=jax.ShapeDtypeStruct((n_tok, hidden), tokens.dtype),
            in_specs=[anywhere, vmem, vmem] + [anywhere] * 6,
            out_specs=vmem,
            scratch_shapes=[
                pltpu.VMEM((4, n_tok, hidden), BF16),
                pltpu.VMEM((4, 16, n_tok), F32),
                pltpu.VMEM((RING, hidden, ff), BF16),
                pltpu.VMEM((GROUP, rows, hidden), BF16),
                pltpu.VMEM((n_exp, rows, ff), BF16),
                pltpu.VMEM((2, n_tok, ff), BF16),
                pltpu.VMEM((4, n_tok, 3 * n_exp * cap), BF16),
                pltpu.VMEM((4, n_exp * cap, CHUNK), BF16),
                pltpu.VMEM((n_tok, 128), F32),
                pltpu.VMEM((n_chunks,) + block, F32),
                pltpu.VMEM((2,) + block, F32),
                pltpu.VMEM((2,) + block, F32),
                pltpu.VMEM((n_chunks,) + block, F32),
                pltpu.VMEM((n_chunks,) + block, F32),
                pltpu.VMEM((n_chunks,) + block, F32),
                dma, dma((RING,)), dma((RING * per_slot,)),
                dma((2 * PIECES + 1,)), dma((2 * PIECES + 1,)), dma((4,)), dma((4,)),
                dma((2,)), dma((2,)), dma((n_chunks,)),
                dma((n_chunks,)), dma((n_chunks,)), dma((n_chunks,)),
            ],
            compiler_params=pltpu.CompilerParams(collective_id=0, has_side_effects=True, vmem_limit_bytes=67043328),
        )(tokens, route, shared_gate.reshape(1, hidden), shared_w1, shared_w3, shared_w2, expert_w1, expert_w3, expert_w2)

    return jax.shard_map(device_step, mesh=mesh, in_specs=(row_spec, row_spec, row_spec, row_spec, P(), P(), P(), P(), expert_spec, expert_spec, expert_spec), out_specs=row_spec, check_vma=False)
```

```python
import functools

import jax
import jax.numpy as jnp
from jax import lax
from jax.experimental import pallas as pl
from jax.experimental.pallas import tpu as pltpu
from jax.sharding import PartitionSpec as P

MESH = pl.DeviceIdType.MESH
F32 = jnp.float32
BF16 = jnp.bfloat16
CHUNK = 256
RING = 5
PIECES = 4
GROUP = 4
LAG = 2
BATCH = 8
BF16_MAX = 3.3895313892515355e38


def moe_kernel(cfg, tok, route, sgate, sw1, sw3, sw2, ew1, ew3, ew2, y,
               toks, rts, wbuf, xg, h, hs, gs, rbuf, sig, acc, send3, send1, recv3, recv1, recvu,
               load_sem, wsem, tsem, tok_send, tok_recv, rt_send, rt_recv,
               s3_send, s1_send, su_send, r3_sem, r1_sem, ru_sem):
    n_tok, hidden, n_exp, ff, cap, top_k = cfg
    n_chunks = hidden // CHUNK
    per_slot = ff // CHUNK
    n_sub = RING * per_slot
    n_items = 2 * (n_exp + 2)
    per_chunk = n_exp + 2
    n_tiles = n_chunks * per_chunk
    piece = n_tok // PIECES
    slots_all = n_exp * cap

    dp = lax.axis_index('dp')
    me = lax.axis_index('ep')
    partner = (dp, me + 1 - 2 * lax.rem(me, 2))
    across = (dp, lax.rem(me + 2, 4))
    diagonal = (dp, 3 - me)

    def shared_item(item):
        src = (sw1, sw3)[item % 2].at[:, pl.ds((item // 2) * ff, ff)]
        return pltpu.make_async_copy(src, wbuf.at[item % RING], wsem.at[item % RING])

    def expert_item(exp, which):
        slot = lax.rem(2 * exp + 4 + which, RING)
        return pltpu.make_async_copy((ew1, ew3)[which].at[exp], wbuf.at[slot], wsem.at[slot])

    def tile_dst(tile):
        sub = lax.rem(tile, n_sub)
        slot = lax.rem(1 + sub // per_slot, RING)
        lane = pl.multiple_of(lax.rem(sub, per_slot) * CHUNK, CHUNK)
        return slot, lane, sub

    def tile_view(tile):
        slot, lane, sub = tile_dst(tile)
        return wbuf.at[slot, pl.ds(0, ff), pl.ds(lane, CHUNK)], tsem.at[sub]

    def start_tile(tile):
        chunk, idx = tile // per_chunk, lax.rem(tile, per_chunk)
        col = pl.ds(pl.multiple_of(chunk * CHUNK, CHUNK), CHUNK)
        dst, sem = tile_view(tile)

        @pl.when(idx < n_exp)
        def _():
            pltpu.make_async_copy(ew2.at[idx, :, col], dst, sem).start()

        @pl.when(idx >= n_exp)
        def _():
            row = pl.multiple_of((idx - n_exp) * ff, 128)
            pltpu.make_async_copy(sw2.at[pl.ds(row, ff), col], dst, sem).start()

    def wait_tile(tile):
        dst, sem = tile_view(tile)
        pltpu.make_async_copy(ew2.at[0, :, pl.ds(0, CHUNK)], dst, sem).wait()

    def load_tile(tile):
        slot, lane, _ = tile_dst(tile)
        return wbuf[slot, pl.ds(0, ff), pl.ds(lane, CHUNK)]

    own_load = pltpu.make_async_copy(tok, toks.at[0], load_sem)
    own_load.start()
    barrier = pltpu.get_barrier_semaphore()
    for peer in (partner, across, diagonal):
        pl.semaphore_signal(barrier, inc=1, device_id=peer, device_id_type=MESH)
    with jax.named_scope('own_load'):
        own_load.wait()
    for item in range(4):
        shared_item(item).start()
    expert_item(0, 0).start()
    with jax.named_scope('barrier'):
        pl.semaphore_wait(barrier, 3)

    def remote(src, dst, send, recv, peer):
        return pltpu.make_async_remote_copy(src_ref=src, dst_ref=dst, send_sem=send, recv_sem=recv,
                                            device_id=peer, device_id_type=MESH)

    def piece_of(ref, i):
        return ref.at[pl.ds(i * piece, piece)]

    rt_copies = [remote(route, rts.at[d], rt_send.at[d], rt_recv.at[d], peer)
                 for d, peer in ((1, partner), (2, across), (3, diagonal))]
    for copy in rt_copies:
        copy.start()
    tok_across = [remote(piece_of(toks.at[0], i), piece_of(toks.at[2], i), tok_send.at[i], tok_recv.at[i], across)
                  for i in range(PIECES)]
    for copy in tok_across:
        copy.start()
    tok_partner = remote(toks.at[0], toks.at[1], tok_send.at[2 * PIECES], tok_recv.at[2 * PIECES], partner)
    tok_partner.start()
    tok_relay = [remote(piece_of(toks.at[2], i), piece_of(toks.at[3], i), tok_send.at[PIECES + i],
                        tok_recv.at[PIECES + i], partner) for i in range(PIECES)]

    def swiglu_cols(x, slot1, slot3, store):
        for i in range(per_slot):
            col = i * CHUNK
            a = jnp.dot(x(), wbuf[slot1, :, pl.ds(col, CHUNK)], preferred_element_type=F32)
            b = jnp.dot(x(), wbuf[slot3, :, pl.ds(col, CHUNK)], preferred_element_type=F32)
            store(col, CHUNK, (jax.nn.silu(a) * b).astype(BF16))
        done = per_slot * CHUNK
        rest = ff - done
        w = jnp.concatenate([wbuf[slot1, :, pl.ds(done, rest)], wbuf[slot3, :, pl.ds(done, rest)]], axis=1)
        ab = jnp.dot(x(), w, preferred_element_type=F32)
        store(done, rest, (jax.nn.silu(ab[:, :rest]) * ab[:, rest:]).astype(BF16))

    for half in range(2):
        shared_item(2 * half).wait()
        shared_item(2 * half + 1).wait()

        def store_shared(col, width, value):
            hs[half, :, pl.ds(col, width)] = value

        swiglu_cols(lambda: toks[0], (2 * half) % RING, (2 * half + 1) % RING, store_shared)
        expert_item(half, 1).start()
        expert_item(half + 1, 0).start()

    logit = jnp.sum(toks[0].astype(F32) * sgate[...].astype(F32), axis=1, keepdims=True)
    sig[...] = jnp.broadcast_to(jax.nn.sigmoid(logit), sig.shape)

    for copy in rt_copies:
        copy.wait_recv()
    tok_partner.wait_recv()
    base = (me * slots_all).astype(F32)

    def route_rows(d):
        return route if d == 0 else rts.at[d]

    for d in range(4):
        def weight_block(i, carry):
            row = (lax.broadcasted_iota(jnp.int32, (128, n_tok), 0) + i * 128).astype(F32) + base
            g = jnp.zeros((128, n_tok), F32)
            for k in range(top_k):
                g += jnp.where(row == route_rows(d)[k:k + 1, :], route_rows(d)[8 + k:9 + k, :], 0.0)
            g = g.T
            g1 = jnp.minimum(g, BF16_MAX).astype(BF16)
            left = g - g1.astype(F32)
            g2 = left.astype(BF16)
            g3 = (left - g2.astype(F32)).astype(BF16)
            for part, value in enumerate((g1, g2, g3)):
                gs[d, :, pl.ds(pl.multiple_of(part * slots_all + i * 128, 128), 128)] = value
            return carry
        lax.fori_loop(0, slots_all // 128, weight_block, 0)

    for arrived, relay in zip(tok_across, tok_relay):
        arrived.wait_recv()
        relay.start()
    for relay in tok_relay:
        relay.wait_recv()

    def group_step(g, carry):
        for d in range(4):
            row = (lax.broadcasted_iota(jnp.int32, (GROUP * cap, n_tok), 0) + g * (GROUP * cap)).astype(F32) + base
            pick = jnp.zeros((GROUP * cap, n_tok), F32)
            for k in range(top_k):
                pick += jnp.where(row == route_rows(d)[k:k + 1, :], 1.0, 0.0)
            pick = pick.astype(BF16)

            for i in range(hidden // 512):
                col = pl.ds(i * 512, 512)
                got = jnp.dot(pick, toks[d, :, col], preferred_element_type=F32).astype(BF16)
                for e in range(GROUP):
                    xg[e, pl.ds(d * cap, cap), col] = got[e * cap:(e + 1) * cap]

        def expert_step(i, carry):
            exp = g * GROUP + i
            expert_item(exp, 0).wait()
            expert_item(exp, 1).wait()

            def store_h(col, width, value):
                h[exp, :, pl.ds(col, width)] = value

            slot1, slot3 = lax.rem(2 * exp + 4, RING), lax.rem(2 * exp + 5, RING)
            swiglu_cols(lambda: xg[i], slot1, slot3, store_h)

            @pl.when(exp + 2 < n_exp)
            def _():
                expert_item(exp + 2, 1).start()

            @pl.when(exp + 3 < n_exp)
            def _():
                expert_item(exp + 3, 0).start()

            @pl.when(exp == n_exp - 3)
            def _():
                for t in range(per_slot):
                    start_tile(jnp.int32(t))

            @pl.when(exp == n_exp - 2)
            def _():
                for t in range(per_slot, 3 * per_slot):
                    start_tile(jnp.int32(t))

            @pl.when(exp == n_exp - 1)
            def _():
                for t in range(3 * per_slot, 5 * per_slot):
                    start_tile(jnp.int32(t))
            return carry
        lax.fori_loop(0, GROUP, expert_step, 0)
        return carry
    lax.fori_loop(0, n_exp // GROUP, group_step, 0)

    def next_tile(tile):
        @pl.when(tile + n_sub < n_tiles)
        def _():
            start_tile(tile + n_sub)

    def combine(d):
        r = rbuf[d]
        return jnp.dot(gs[d], jnp.concatenate([r, r, r], axis=0), preferred_element_type=F32)

    def to_partner3(j):
        return remote(send3.at[lax.rem(j, 2)], recv3.at[j], s3_send.at[lax.rem(j, 2)], r3_sem.at[j], partner)

    def to_partner1(j):
        return remote(send1.at[lax.rem(j, 2)], recv1.at[j], s1_send.at[lax.rem(j, 2)], r1_sem.at[j], partner)

    def to_across(j):
        return remote(recv3.at[j], recvu.at[j], su_send.at[j], ru_sem.at[j], across)

    def finish(j):
        to_partner1(j).wait_recv()
        to_across(j).wait_recv()
        col = pl.ds(pl.multiple_of(j * CHUNK, CHUNK), CHUNK)
        y[:, col] = (acc[j] + recv1[j] + recvu[j]).astype(y.dtype)

    def chunk_step(j, carry):
        first = j * per_chunk

        def batch_step(i, carry):
            tile = first + BATCH * i
            for u in range(BATCH):
                wait_tile(tile + u)
            for u in range(BATCH):
                exp = BATCH * i + u
                r = jnp.dot(h[exp], load_tile(tile + u), preferred_element_type=F32).astype(BF16)
                for d in range(4):
                    rbuf[d, pl.ds(pl.multiple_of(exp * cap, 16), cap), :] = r[d * cap:(d + 1) * cap]
            for u in range(BATCH):
                next_tile(tile + u)
            return carry
        lax.fori_loop(0, n_exp // BATCH, batch_step, 0)

        @pl.when(j >= 2)
        def _():
            to_partner3(j - 2).wait_send()
            to_partner1(j - 2).wait_send()
        tile = first + n_exp
        wait_tile(tile)
        wait_tile(tile + 1)
        send3[lax.rem(j, 2)] = combine(3)
        send1[lax.rem(j, 2)] = combine(1)
        to_partner3(j).start()
        to_partner1(j).start()
        part2 = combine(2)
        s = (jnp.dot(hs[0], load_tile(tile), preferred_element_type=F32)
             + jnp.dot(hs[1], load_tile(tile + 1), preferred_element_type=F32))
        col = pl.ds(pl.multiple_of(j * CHUNK, CHUNK), CHUNK)
        acc[j] = toks[0, :, col].astype(F32) + sig[:, 0:1] * s + combine(0)
        to_partner3(j).wait_recv()
        recv3[j] = recv3[j] + part2
        to_across(j).start()
        next_tile(tile)
        next_tile(tile + 1)

        @pl.when(j >= LAG)
        def _():
            finish(j - LAG)
        return carry
    lax.fori_loop(0, n_chunks, chunk_step, 0)

    def last_step(j, carry):
        finish(j)
        return carry
    lax.fori_loop(n_chunks - LAG, n_chunks, last_step, 0)

    for copy in rt_copies + tok_across + tok_relay + [tok_partner]:
        copy.wait_send()
    for j in range(n_chunks - 2, n_chunks):
        to_partner3(j).wait_send()
        to_partner1(j).wait_send()

    def drain(j, carry):
        to_across(j).wait_send()
        return carry
    lax.fori_loop(0, n_chunks, drain, 0)


def solution(mesh):
    num_ep = mesh.shape['ep']
    row_spec = P(('dp', 'ep'), None)
    expert_spec = P('ep', None, None)

    def device_step(tokens, expert_ids, gate_vals, slots, shared_w1, shared_w3, shared_w2, shared_gate, expert_w1, expert_w3, expert_w2):
        n_tok, hidden = tokens.shape
        top_k = expert_ids.shape[1]
        n_exp, _, ff = expert_w1.shape
        num_experts = n_exp * num_ep
        cap = 8 * ((2 * n_tok * top_k + 8 * num_experts - 1) // (8 * num_experts))
        rows = num_ep * cap
        n_chunks = hidden // CHUNK
        per_slot = ff // CHUNK

        dest = jnp.where(slots >= 0, expert_ids * cap + slots, -1).astype(F32)
        pad = ((0, 8 - top_k), (0, 0))
        route = jnp.concatenate([jnp.pad(dest.T, pad, constant_values=-1.0), jnp.pad(gate_vals.T, pad)], axis=0)

        anywhere = pl.BlockSpec(memory_space=pl.ANY)
        vmem = pl.BlockSpec(memory_space=pltpu.VMEM)
        dma = pltpu.SemaphoreType.DMA
        block = (n_tok, CHUNK)
        return pl.pallas_call(
            functools.partial(moe_kernel, (n_tok, hidden, n_exp, ff, cap, top_k)),
            out_shape=jax.ShapeDtypeStruct((n_tok, hidden), tokens.dtype),
            in_specs=[anywhere, vmem, vmem] + [anywhere] * 6,
            out_specs=vmem,
            scratch_shapes=[
                pltpu.VMEM((4, n_tok, hidden), BF16),
                pltpu.VMEM((4, 16, n_tok), F32),
                pltpu.VMEM((RING, hidden, ff), BF16),
                pltpu.VMEM((GROUP, rows, hidden), BF16),
                pltpu.VMEM((n_exp, rows, ff), BF16),
                pltpu.VMEM((2, n_tok, ff), BF16),
                pltpu.VMEM((4, n_tok, 3 * n_exp * cap), BF16),
                pltpu.VMEM((4, n_exp * cap, CHUNK), BF16),
                pltpu.VMEM((n_tok, 128), F32),
                pltpu.VMEM((n_chunks,) + block, F32),
                pltpu.VMEM((2,) + block, F32),
                pltpu.VMEM((2,) + block, F32),
                pltpu.VMEM((n_chunks,) + block, F32),
                pltpu.VMEM((n_chunks,) + block, F32),
                pltpu.VMEM((n_chunks,) + block, F32),
                dma, dma((RING,)), dma((RING * per_slot,)),
                dma((2 * PIECES + 1,)), dma((2 * PIECES + 1,)), dma((4,)), dma((4,)),
                dma((2,)), dma((2,)), dma((n_chunks,)),
                dma((n_chunks,)), dma((n_chunks,)), dma((n_chunks,)),
            ],
            compiler_params=pltpu.CompilerParams(collective_id=0, has_side_effects=True, vmem_limit_bytes=67043328),
        )(tokens, route, shared_gate.reshape(1, hidden), shared_w1, shared_w3, shared_w2, expert_w1, expert_w3, expert_w2)

    return jax.shard_map(device_step, mesh=mesh, in_specs=(row_spec, row_spec, row_spec, row_spec, P(), P(), P(), P(), expert_spec, expert_spec, expert_spec), out_specs=row_spec, check_vma=False)
```

```python
import functools

import jax
import jax.numpy as jnp
from jax import lax
from jax.experimental import pallas as pl
from jax.experimental.pallas import tpu as pltpu
from jax.sharding import PartitionSpec as P

MESH = pl.DeviceIdType.MESH
F32 = jnp.float32
BF16 = jnp.bfloat16
CHUNK = 256
BLOCK = 512
RING = 3
PIECES = 8
GROUP = 4
BATCH = 8
LAG = 2
BF16_MAX = 3.3895313892515355e38


def moe_kernel(cfg, tok, ids, slots, gates, sgate, sw1, sw3, sw2, ew1, ew3, ew2, y,
               toks, ids_v, slots_v, gates_v, sgate_v, rts, wbuf, xg, h, gs, rbuf, sig, acc,
               send3, send1, recv3, recv1, recvu,
               load_sem, wsem, tsem, tok_send, tok_recv, rt_send, rt_recv,
               s3_send, s1_send, su_send, r3_sem, r1_sem, ru_sem):
    n_tok, hidden, n_exp, ff, cap, top_k = cfg
    rows = 4 * cap
    n_chunks = hidden // CHUNK
    offsets = list(range(0, ff, BLOCK))
    widths = [min(BLOCK, ff - o) for o in offsets]
    n_blocks = len(offsets)
    per_place = 2 * (ff // CHUNK)
    n_sub = RING * per_place
    n_tiles = n_chunks * n_exp
    piece = n_tok // PIECES
    slots_all = n_exp * cap

    dp = lax.axis_index('dp')
    me = lax.axis_index('ep')
    partner = (dp, me + 1 - 2 * lax.rem(me, 2))
    across = (dp, lax.rem(me + 2, 4))
    diagonal = (dp, 3 - me)

    def block_copies(n, srcs, b):
        place = n % RING if isinstance(n, int) else lax.rem(n, RING)
        col = pl.ds(offsets[b], widths[b])
        return [pltpu.make_async_copy(src, wbuf.at[place, i, :, col], wsem.at[place, i, b]) for i, src in enumerate(srcs)]

    def shared_block(half, b):
        col = pl.ds(half * ff + offsets[b], widths[b])
        return block_copies(half, (sw1.at[:, col], sw3.at[:, col]), b)

    def expert_block(exp, b):
        col = pl.ds(offsets[b], widths[b])
        return block_copies(exp + 2, (ew1.at[exp, :, col], ew3.at[exp, :, col]), b)

    def start(copies):
        for copy in copies:
            copy.start()

    def wait(copies):
        for copy in copies:
            copy.wait()

    def tiles_in(b):
        return range(offsets[b] // CHUNK * 2, (offsets[b] + widths[b]) // CHUNK * 2)

    def start_after(exp, b):
        @pl.when(exp + RING < n_exp)
        def _():
            start(expert_block(exp + RING, b))

        @pl.when(exp + RING >= n_exp)
        def _():
            for t in tiles_in(b):
                start_tile((exp + RING - n_exp) * per_place + t)

    def tile_place(tile):
        sub = lax.rem(tile, n_sub)
        place = lax.rem(n_exp + 2 + sub // per_place, RING)
        r = lax.rem(sub, per_place)
        lane = pl.multiple_of(r // 2 * CHUNK, CHUNK)
        return (place, lax.rem(r, 2), pl.ds(0, ff), pl.ds(lane, CHUNK)), sub

    def tile_copy(tile):
        where, sub = tile_place(tile)
        chunk, exp = tile // n_exp, lax.rem(tile, n_exp)
        col = pl.ds(pl.multiple_of(chunk * CHUNK, CHUNK), CHUNK)
        return pltpu.make_async_copy(ew2.at[exp, :, col], wbuf.at[where], tsem.at[sub])

    def start_tile(tile):
        tile_copy(tile).start()

    def next_tile(tile):
        @pl.when(tile + n_sub < n_tiles)
        def _():
            start_tile(tile + n_sub)

    n_held = (n_exp * rows // ff) * (ff // CHUNK)

    def shared_place(tile):
        if tile < n_held:
            row, lane = divmod(tile, ff // CHUNK)
            return h.at[pl.ds(row * ff, ff), pl.ds(lane * CHUNK, CHUNK)]
        lane, which = divmod(tile - n_held, 2)
        return wbuf.at[0, which, pl.ds(0, ff), pl.ds(lane * CHUNK, CHUNK)]

    def shared_tile(tile):
        chunk, half = divmod(tile, 2)
        return pltpu.make_async_copy(sw2.at[pl.ds(half * ff, ff), pl.ds(chunk * CHUNK, CHUNK)],
                                     shared_place(tile), tsem.at[tile])

    def remote(src, dst, send, recv, peer):
        return pltpu.make_async_remote_copy(src_ref=src, dst_ref=dst, send_sem=send, recv_sem=recv,
                                            device_id=peer, device_id_type=MESH)

    loads = [pltpu.make_async_copy(src, dst, load_sem.at[i]) for i, (src, dst) in enumerate(
        ((ids, ids_v), (slots, slots_v), (gates, gates_v), (sgate, sgate_v), (tok, toks.at[0])))]
    start(loads)
    barrier = pltpu.get_barrier_semaphore()
    for peer in (partner, across, diagonal):
        pl.semaphore_signal(barrier, inc=1, device_id=peer, device_id_type=MESH)
    with jax.named_scope('own_load'):
        wait(loads)
    start(shared_block(0, 0))
    dest = jnp.where(slots_v[...] >= 0, ids_v[...] * cap + slots_v[...], -1).astype(F32)
    rts[0] = jnp.zeros_like(rts[0])
    rts[0, 0:top_k, :] = dest
    rts[0, 8:8 + top_k, :] = gates_v[...]
    with jax.named_scope('barrier'):
        pl.semaphore_wait(barrier, 3)

    def piece_of(ref, i):
        return ref.at[pl.ds(i * piece, piece)]

    tok_across = [remote(piece_of(toks.at[0], i), piece_of(toks.at[2], i), tok_send.at[i], tok_recv.at[i], across)
                  for i in range(PIECES)]
    tok_partner = remote(toks.at[0], toks.at[1], tok_send.at[2 * PIECES], tok_recv.at[2 * PIECES], partner)
    rt_copies = [remote(rts.at[0], rts.at[d], rt_send.at[d], rt_recv.at[d], peer)
                 for d, peer in ((1, partner), (2, across), (3, diagonal))]
    start(rt_copies + tok_across + [tok_partner])
    for half in range(2):
        for b in range(n_blocks):
            if (half, b) != (0, 0):
                start(shared_block(half, b))
    for tile in range(n_held):
        shared_tile(tile).start()
    for b in range(n_blocks):
        start(expert_block(0, b))
    tok_relay = [remote(piece_of(toks.at[2], i), piece_of(toks.at[3], i), tok_send.at[PIECES + i],
                        tok_recv.at[PIECES + i], partner) for i in range(PIECES)]

    def relay(begin, end):
        for i in range(begin, end):
            tok_across[i].wait_recv()
            tok_relay[i].start()

    def swiglu_block(x, place, b, store):
        done = 0
        while done < widths[b]:
            width = min(CHUNK, widths[b] - done)
            if width == CHUNK:
                a = jnp.dot(x(), wbuf[place, 0, :, pl.ds(offsets[b] + done, width)], preferred_element_type=F32)
                g = jnp.dot(x(), wbuf[place, 1, :, pl.ds(offsets[b] + done, width)], preferred_element_type=F32)
            else:
                w = jnp.concatenate([wbuf[place, 0, :, pl.ds(offsets[b] + done, width)], wbuf[place, 1, :, pl.ds(offsets[b] + done, width)]], axis=1)
                both = jnp.dot(x(), w, preferred_element_type=F32)
                a, g = both[:, :width], both[:, width:]
            store(offsets[b] + done, width, (jax.nn.silu(a) * g).astype(BF16))
            done += width

    with jax.named_scope('shared'):
        for half in range(2):
            for b in range(n_blocks):
                wait(shared_block(half, b))

                def store_shared(col, width, value):
                    xg[pl.ds(half * n_tok, n_tok), pl.ds(col, width)] = value

                swiglu_block(lambda: toks[0], half, b, store_shared)
                if half == 0:
                    for t in tiles_in(b):
                        if n_held + t < 2 * n_chunks:
                            shared_tile(n_held + t).start()

    total = jnp.zeros((n_tok, 128), F32)
    for i in range(hidden // 128):
        total += toks[0, :, pl.ds(i * 128, 128)].astype(F32) * sgate_v[i:i + 1, :].astype(F32)
    logit = jnp.sum(total, axis=1, keepdims=True)
    sig[...] = jnp.broadcast_to(jax.nn.sigmoid(logit), sig.shape)

    with jax.named_scope('shared2'):
        for tile in range(2 * n_chunks):
            shared_tile(tile).wait()
        for chunk in range(n_chunks):
            s = sum(jnp.dot(xg[pl.ds(half * n_tok, n_tok), pl.ds(0, ff)], shared_place(2 * chunk + half)[...],
                            preferred_element_type=F32) for half in range(2))
            acc[chunk] = toks[0, :, pl.ds(chunk * CHUNK, CHUNK)].astype(F32) + sig[:, 0:1] * s
        for exp in range(1, RING):
            for b in range(n_blocks):
                start(expert_block(exp, b))

    relay(0, PIECES // 2)
    with jax.named_scope('wait_near'):
        for copy in rt_copies:
            copy.wait_recv()
        tok_partner.wait_recv()
    base = (me * slots_all).astype(F32)

    with jax.named_scope('weights'):
        for d in range(4):
            def weight_block(i, carry):
                row = (lax.broadcasted_iota(jnp.int32, (128, n_tok), 0) + i * 128).astype(F32) + base
                g = jnp.zeros((128, n_tok), F32)
                for k in range(top_k):
                    g += jnp.where(row == rts[d, k:k + 1, :], rts[d, 8 + k:9 + k, :], 0.0)
                g = g.T
                g1 = jnp.minimum(g, BF16_MAX).astype(BF16)
                left = g - g1.astype(F32)
                g2 = left.astype(BF16)
                g3 = (left - g2.astype(F32)).astype(BF16)
                for part, value in enumerate((g1, g2, g3)):
                    gs[d, :, pl.ds(pl.multiple_of(part * slots_all + i * 128, 128), 128)] = value
                return carry
            lax.fori_loop(0, slots_all // 128, weight_block, 0)

    def gather(g, sources):
        for d in sources:
            row = (lax.broadcasted_iota(jnp.int32, (GROUP * cap, n_tok), 0) + g * (GROUP * cap)).astype(F32) + base
            pick = jnp.zeros((GROUP * cap, n_tok), F32)
            for k in range(top_k):
                pick += jnp.where(row == rts[d, k:k + 1, :], 1.0, 0.0)
            pick = pick.astype(BF16)
            for i in range(hidden // 512):
                col = pl.ds(i * 512, 512)
                got = jnp.dot(pick, toks[d, :, col], preferred_element_type=F32).astype(BF16)
                for e in range(GROUP):
                    xg[pl.ds(e * rows + d * cap, cap), col] = got[e * cap:(e + 1) * cap]

    with jax.named_scope('gather_near'):
        gather(jnp.int32(0), (0, 1))
    relay(PIECES // 2, PIECES - 2)

    with jax.named_scope('dispatch_wait'):
        relay(PIECES - 2, PIECES)
        gather(jnp.int32(0), (2,))
        for copy in tok_relay:
            copy.wait_recv()

    def keep_rows(exp, r):
        for d in range(4):
            rbuf[d, pl.ds(pl.multiple_of(exp * cap, 16), cap), :] = r[d * cap:(d + 1) * cap]

    def h_rows(exp):
        return pl.ds(pl.multiple_of(exp * rows, rows), rows)

    def group_step(g, carry):
        with jax.named_scope('gather'):
            @pl.when(g == 0)
            def _():
                gather(g, (3,))

            @pl.when(g > 0)
            def _():
                gather(g, range(4))

        def expert_step(i, carry):
            exp = g * GROUP + i
            x_rows = pl.ds(pl.multiple_of(i * rows, rows), rows)

            def store_h(col, width, value):
                h[h_rows(exp), pl.ds(col, width)] = value

            def block(b):
                swiglu_block(lambda: xg[x_rows, :], lax.rem(exp + 2, RING), b, store_h)

            edge = (exp == 0) | (exp == n_exp - 1)

            @pl.when(edge)
            def _():
                for b in range(n_blocks):
                    with jax.named_scope('edge_wait'):
                        wait(expert_block(exp, b))
                    with jax.named_scope('edge_block'):
                        block(b)
                        start_after(exp, b)

            @pl.when(jnp.logical_not(edge))
            def _():
                with jax.named_scope('w_wait'):
                    for b in range(n_blocks):
                        wait(expert_block(exp, b))
                with jax.named_scope('expert'):
                    for b in range(n_blocks):
                        block(b)
                    for b in range(n_blocks):
                        start_after(exp, b)
            return carry
        lax.fori_loop(0, GROUP, expert_step, 0)
        return carry
    lax.fori_loop(0, n_exp // GROUP, group_step, 0)

    def combine(d):
        r = rbuf[d]
        return jnp.dot(gs[d], jnp.concatenate([r, r, r], axis=0), preferred_element_type=F32)

    def to_partner3(j):
        return remote(send3.at[lax.rem(j, 2)], recv3.at[lax.rem(j, 4)], s3_send.at[lax.rem(j, 2)], r3_sem.at[j], partner)

    def to_partner1(j):
        return remote(send1.at[lax.rem(j, 2)], recv1.at[lax.rem(j, 4)], s1_send.at[lax.rem(j, 2)], r1_sem.at[j], partner)

    def to_across(j):
        return remote(recv3.at[lax.rem(j, 4)], recvu.at[lax.rem(j, 6)], su_send.at[j], ru_sem.at[j], across)

    def finish(j):
        to_partner1(j).wait_recv()
        to_across(j).wait_recv()
        col = pl.ds(pl.multiple_of(j * CHUNK, CHUNK), CHUNK)
        y[:, col] = (acc[j] + recv1[lax.rem(j, 4)] + recvu[lax.rem(j, 6)]).astype(y.dtype)

    def chunk_step(j, carry):
        def batch_step(i, carry):
            tile = j * n_exp + BATCH * i
            with jax.named_scope('t_wait'):
                for u in range(BATCH):
                    tile_copy(tile + u).wait()
            for u in range(BATCH):
                exp = BATCH * i + u
                keep_rows(exp, jnp.dot(h[h_rows(exp), :], wbuf[tile_place(tile + u)[0]],
                                       preferred_element_type=F32).astype(BF16))
            for u in range(BATCH):
                next_tile(tile + u)
            return carry

        with jax.named_scope('tiles'):
            lax.fori_loop(0, n_exp // BATCH, batch_step, 0)

        @pl.when(j >= 3)
        def _():
            with jax.named_scope('su_wait'):
                to_across(j - 3).wait_send()

        @pl.when(j >= 2)
        def _():
            to_partner3(j - 2).wait_send()
            to_partner1(j - 2).wait_send()

        with jax.named_scope('combine3'):
            send3[lax.rem(j, 2)] = combine(3)
            to_partner3(j).start()
        with jax.named_scope('combine120'):
            part2 = combine(2)
            send1[lax.rem(j, 2)] = combine(1)
            acc[j] = acc[j] + combine(0)
            to_partner1(j).start()
        with jax.named_scope('pwait'):
            to_partner3(j).wait_recv()
            recv3[lax.rem(j, 4)] = recv3[lax.rem(j, 4)] + part2
            to_across(j).start()

        @pl.when(j >= LAG)
        def _():
            with jax.named_scope('finish'):
                finish(j - LAG)
        return carry
    lax.fori_loop(0, n_chunks, chunk_step, 0)

    def last_step(j, carry):
        with jax.named_scope('last'):
            finish(j)
        return carry
    lax.fori_loop(n_chunks - LAG, n_chunks, last_step, 0)

    for copy in rt_copies + tok_across + tok_relay + [tok_partner]:
        copy.wait_send()
    for j in range(n_chunks - 2, n_chunks):
        to_partner3(j).wait_send()
        to_partner1(j).wait_send()
    for j in range(n_chunks - 3, n_chunks):
        to_across(j).wait_send()


def solution(mesh):
    num_ep = mesh.shape['ep']
    row_spec = P(('dp', 'ep'), None)
    expert_spec = P('ep', None, None)

    def device_step(tokens, expert_ids, gate_vals, slots, shared_w1, shared_w3, shared_w2, shared_gate, expert_w1, expert_w3, expert_w2):
        n_tok, hidden = tokens.shape
        top_k = expert_ids.shape[1]
        n_exp, _, ff = expert_w1.shape
        num_experts = n_exp * num_ep
        cap = 8 * ((2 * n_tok * top_k + 8 * num_experts - 1) // (8 * num_experts))
        rows = num_ep * cap
        n_chunks = hidden // CHUNK
        n_sub = RING * 2 * (ff // CHUNK)
        n_blocks = -(-ff // BLOCK)

        anywhere = pl.BlockSpec(memory_space=pl.ANY)
        dma = pltpu.SemaphoreType.DMA
        vm = pltpu.VMEM
        block = (n_tok, CHUNK)
        return pl.pallas_call(
            functools.partial(moe_kernel, (n_tok, hidden, n_exp, ff, cap, top_k)),
            out_shape=jax.ShapeDtypeStruct((n_tok, hidden), tokens.dtype),
            in_specs=[anywhere] * 11,
            out_specs=pl.BlockSpec(memory_space=pltpu.VMEM),
            scratch_shapes=[
                vm((4, n_tok, hidden), BF16),
                vm((top_k, n_tok), jnp.int32), vm((top_k, n_tok), jnp.int32), vm((top_k, n_tok), F32),
                vm((hidden // 128, 128), BF16),
                vm((4, 16, n_tok), F32),
                vm((RING, 2, hidden, ff), BF16),
                vm((GROUP * rows, hidden), BF16),
                vm((n_exp * rows, ff), BF16),
                vm((4, n_tok, 3 * n_exp * cap), BF16),
                vm((4, n_exp * cap, CHUNK), BF16),
                vm((n_tok, 128), F32),
                vm((n_chunks,) + block, F32),
                vm((2,) + block, F32), vm((2,) + block, F32),
                vm((4,) + block, F32), vm((4,) + block, F32), vm((6,) + block, F32),
                dma((5,)), dma((RING, 2, n_blocks)), dma((n_sub,)),
                dma((2 * PIECES + 1,)), dma((2 * PIECES + 1,)), dma((4,)), dma((4,)),
                dma((2,)), dma((2,)), dma((n_chunks,)),
                dma((n_chunks,)), dma((n_chunks,)), dma((n_chunks,)),
            ],
            compiler_params=pltpu.CompilerParams(collective_id=0, has_side_effects=True, vmem_limit_bytes=67043328),
        )(tokens, expert_ids.T, slots.T, gate_vals.T, shared_gate.reshape(hidden // 128, 128),
          shared_w1, shared_w3, shared_w2, expert_w1, expert_w3, expert_w2)

    return jax.shard_map(device_step, mesh=mesh, in_specs=(row_spec, row_spec, row_spec, row_spec, P(), P(), P(), P(), expert_spec, expert_spec, expert_spec), out_specs=row_spec, check_vma=False)
```

```python
import functools

import jax
import jax.numpy as jnp
from jax import lax
from jax.experimental import pallas as pl
from jax.experimental.pallas import tpu as pltpu
from jax.sharding import PartitionSpec as P

MESH = pl.DeviceIdType.MESH
F32 = jnp.float32
BF16 = jnp.bfloat16
CHUNK = 256
BLOCK = 512
RING = 3
PIECES = 8
GROUP = 4
BATCH = 8
LAG = 2
BF16_MAX = 3.3895313892515355e38


def moe_kernel(cfg, tok, ids, slots, gates, sgate, sw1, sw3, sw2, ew1, ew3, ew2, y,
               toks, ids_v, slots_v, gates_v, sgate_v, rts, wbuf, wtail, xg, h, gs, rbuf, sig, acc,
               send3, send1, recv3, recv1, recvu,
               load_sem, wsem, early_sem, tsem, tok_send, tok_recv, rt_send, rt_recv,
               s3_send, s1_send, su_send, r3_sem, r1_sem, ru_sem):
    n_tok, hidden, n_exp, ff, cap, top_k = cfg
    rows = 4 * cap
    n_chunks = hidden // CHUNK
    offsets = list(range(0, ff, BLOCK))
    widths = [min(BLOCK, ff - o) for o in offsets]
    n_blocks = len(offsets)
    per_place = 2 * (ff // CHUNK)
    n_ring = RING * per_place
    n_sub = 2 * n_exp
    piece = n_tok // PIECES
    slots_all = n_exp * cap

    dp = lax.axis_index('dp')
    me = lax.axis_index('ep')
    partner = (dp, me + 1 - 2 * lax.rem(me, 2))
    across = (dp, lax.rem(me + 2, 4))
    diagonal = (dp, 3 - me)

    def block_copies(n, srcs, b, which):
        place = n % RING if isinstance(n, int) else lax.rem(n, RING)
        col = pl.ds(offsets[b], widths[b])
        return [pltpu.make_async_copy(srcs[i], wbuf.at[place, i, :, col], wsem.at[place, i, b]) for i in which]

    def shared_block(half, b):
        col = pl.ds(half * ff + offsets[b], widths[b])
        return block_copies(half, (sw1.at[:, col], sw3.at[:, col]), b, (0, 1))

    def expert_block(exp, b, which=(0, 1)):
        col = pl.ds(offsets[b], widths[b])
        return block_copies(exp + 2, (ew1.at[exp, :, col], ew3.at[exp, :, col]), b, which)

    def start(copies):
        for copy in copies:
            copy.start()

    def wait(copies):
        for copy in copies:
            copy.wait()

    def tiles_in(b):
        return range(offsets[b] // CHUNK * 2, (offsets[b] + widths[b]) // CHUNK * 2)

    def start_after(exp, b):
        @pl.when(exp + RING < n_exp)
        def _():
            start(expert_block(exp + RING, b))

        for later in range(RING):
            @pl.when(exp == n_exp - RING + later)
            def _():
                for t in tiles_in(b):
                    start_tile(later * per_place + t)

    early_rows = pl.ds(n_exp * rows - hidden, hidden)

    def early_block(b):
        col = pl.ds(offsets[b], widths[b])
        return pltpu.make_async_copy(ew1.at[RING, :, col], h.at[early_rows, col], early_sem.at[b])

    def tile_place(sub):
        if sub >= n_ring:
            return wtail.at[sub - n_ring]
        place, r = divmod(sub, per_place)
        return wbuf.at[(n_exp + 2 + place) % RING, r % 2, pl.ds(0, ff), pl.ds(r // 2 * CHUNK, CHUNK)]

    def tile_copy(sub, chunk):
        col = pl.ds(pl.multiple_of(chunk * CHUNK, CHUNK), CHUNK)
        return pltpu.make_async_copy(ew2.at[sub % n_exp, :, col], tile_place(sub), tsem.at[sub])

    def start_tile(sub):
        tile_copy(sub, sub // n_exp).start()

    n_held = (n_exp * rows // ff) * (ff // CHUNK)

    def shared_place(tile):
        if tile < n_held:
            row, lane = divmod(tile, ff // CHUNK)
            return h.at[pl.ds(row * ff, ff), pl.ds(lane * CHUNK, CHUNK)]
        lane, which = divmod(tile - n_held, 2)
        return wbuf.at[0, which, pl.ds(0, ff), pl.ds(lane * CHUNK, CHUNK)]

    def shared_tile(tile):
        chunk, half = divmod(tile, 2)
        return pltpu.make_async_copy(sw2.at[pl.ds(half * ff, ff), pl.ds(chunk * CHUNK, CHUNK)],
                                     shared_place(tile), tsem.at[tile])

    def remote(src, dst, send, recv, peer):
        return pltpu.make_async_remote_copy(src_ref=src, dst_ref=dst, send_sem=send, recv_sem=recv,
                                            device_id=peer, device_id_type=MESH)

    loads = [pltpu.make_async_copy(src, dst, load_sem.at[i]) for i, (src, dst) in enumerate(
        ((ids, ids_v), (slots, slots_v), (gates, gates_v), (sgate, sgate_v), (tok, toks.at[0])))]
    start(loads)
    barrier = pltpu.get_barrier_semaphore()
    for peer in (partner, across, diagonal):
        pl.semaphore_signal(barrier, inc=1, device_id=peer, device_id_type=MESH)
    with jax.named_scope('own_load'):
        wait(loads)
    start(shared_block(0, 0))
    dest = jnp.where(slots_v[...] >= 0, ids_v[...] * cap + slots_v[...], -1).astype(F32)
    rts[0] = jnp.zeros_like(rts[0])
    rts[0, 0:top_k, :] = dest
    rts[0, 8:8 + top_k, :] = gates_v[...]
    with jax.named_scope('barrier'):
        pl.semaphore_wait(barrier, 3)

    def piece_of(ref, i):
        return ref.at[pl.ds(i * piece, piece)]

    tok_across = [remote(piece_of(toks.at[0], i), piece_of(toks.at[2], i), tok_send.at[i], tok_recv.at[i], across)
                  for i in range(PIECES)]
    tok_partner = remote(toks.at[0], toks.at[1], tok_send.at[2 * PIECES], tok_recv.at[2 * PIECES], partner)
    rt_copies = [remote(rts.at[0], rts.at[d], rt_send.at[d], rt_recv.at[d], peer)
                 for d, peer in ((1, partner), (2, across), (3, diagonal))]
    start(rt_copies + tok_across + [tok_partner])
    for half in range(2):
        for b in range(n_blocks):
            if (half, b) != (0, 0):
                start(shared_block(half, b))
    for tile in range(n_held):
        shared_tile(tile).start()
    for b in range(n_blocks):
        start(expert_block(0, b))
    tok_relay = [remote(piece_of(toks.at[2], i), piece_of(toks.at[3], i), tok_send.at[PIECES + i],
                        tok_recv.at[PIECES + i], partner) for i in range(PIECES)]

    def relay(begin, end):
        for i in range(begin, end):
            tok_across[i].wait_recv()
            tok_relay[i].start()

    def swiglu_block(x, w1, w3, b, store):
        done = 0
        while done < widths[b]:
            width = min(CHUNK, widths[b] - done)
            if width == CHUNK:
                a = jnp.dot(x(), w1[:, pl.ds(offsets[b] + done, width)], preferred_element_type=F32)
                g = jnp.dot(x(), w3[:, pl.ds(offsets[b] + done, width)], preferred_element_type=F32)
            else:
                w = jnp.concatenate([w1[:, pl.ds(offsets[b] + done, width)], w3[:, pl.ds(offsets[b] + done, width)]], axis=1)
                both = jnp.dot(x(), w, preferred_element_type=F32)
                a, g = both[:, :width], both[:, width:]
            store(offsets[b] + done, width, (jax.nn.silu(a) * g).astype(BF16))
            done += width

    with jax.named_scope('shared'):
        for half in range(2):
            for b in range(n_blocks):
                wait(shared_block(half, b))

                def store_shared(col, width, value):
                    xg[pl.ds(half * n_tok, n_tok), pl.ds(col, width)] = value

                swiglu_block(lambda: toks[0], wbuf.at[half, 0], wbuf.at[half, 1], b, store_shared)
                if half == 0:
                    for t in tiles_in(b):
                        if n_held + t < 2 * n_chunks:
                            shared_tile(n_held + t).start()

    total = jnp.zeros((n_tok, 128), F32)
    for i in range(hidden // 128):
        total += toks[0, :, pl.ds(i * 128, 128)].astype(F32) * sgate_v[i:i + 1, :].astype(F32)
    logit = jnp.sum(total, axis=1, keepdims=True)
    sig[...] = jnp.broadcast_to(jax.nn.sigmoid(logit), sig.shape)

    with jax.named_scope('shared2'):
        for b in range(n_blocks):
            start(expert_block(2, b))
        for chunk in range(n_chunks):
            for half in range(2):
                shared_tile(2 * chunk + half).wait()
            s = sum(jnp.dot(xg[pl.ds(half * n_tok, n_tok), pl.ds(0, ff)], shared_place(2 * chunk + half)[...],
                            preferred_element_type=F32) for half in range(2))
            acc[chunk] = toks[0, :, pl.ds(chunk * CHUNK, CHUNK)].astype(F32) + sig[:, 0:1] * s
        for b in range(n_blocks):
            start(expert_block(1, b))
        for b in range(n_blocks):
            early_block(b).start()

    relay(0, PIECES // 2)
    with jax.named_scope('wait_near'):
        for copy in rt_copies:
            copy.wait_recv()
        tok_partner.wait_recv()
    base = (me * slots_all).astype(F32)

    with jax.named_scope('weights'):
        for d in range(4):
            def weight_block(i, carry):
                row = (lax.broadcasted_iota(jnp.int32, (128, n_tok), 0) + i * 128).astype(F32) + base
                g = jnp.zeros((128, n_tok), F32)
                for k in range(top_k):
                    g += jnp.where(row == rts[d, k:k + 1, :], rts[d, 8 + k:9 + k, :], 0.0)
                g = g.T
                g1 = jnp.minimum(g, BF16_MAX).astype(BF16)
                left = g - g1.astype(F32)
                g2 = left.astype(BF16)
                g3 = (left - g2.astype(F32)).astype(BF16)
                for part, value in enumerate((g1, g2, g3)):
                    gs[d, :, pl.ds(pl.multiple_of(part * slots_all + i * 128, 128), 128)] = value
                return carry
            lax.fori_loop(0, slots_all // 128, weight_block, 0)

    def gather(g, sources):
        for d in sources:
            row = (lax.broadcasted_iota(jnp.int32, (GROUP * cap, n_tok), 0) + g * (GROUP * cap)).astype(F32) + base
            pick = jnp.zeros((GROUP * cap, n_tok), F32)
            for k in range(top_k):
                pick += jnp.where(row == rts[d, k:k + 1, :], 1.0, 0.0)
            pick = pick.astype(BF16)
            for i in range(hidden // 512):
                col = pl.ds(i * 512, 512)
                got = jnp.dot(pick, toks[d, :, col], preferred_element_type=F32).astype(BF16)
                for e in range(GROUP):
                    xg[pl.ds(e * rows + d * cap, cap), col] = got[e * cap:(e + 1) * cap]

    with jax.named_scope('gather_near'):
        gather(jnp.int32(0), (0, 1))
    relay(PIECES // 2, PIECES - 2)

    with jax.named_scope('dispatch_wait'):
        relay(PIECES - 2, PIECES)
        gather(jnp.int32(0), (2,))
        for copy in tok_relay:
            copy.wait_recv()

    def h_rows(exp):
        return pl.ds(exp * rows if isinstance(exp, int) else pl.multiple_of(exp * rows, rows), rows)

    def group_step(g, carry):
        with jax.named_scope('gather'):
            @pl.when(g == 0)
            def _():
                gather(g, (3,))

            @pl.when(g > 0)
            def _():
                gather(g, range(4))

        def expert_step(i, carry):
            exp = g * GROUP + i
            place = lax.rem(exp + 2, RING)

            def whole(e, slot, w1):
                x_rows = pl.ds(pl.multiple_of(i * rows, rows), rows)

                def store_h(col, width, value):
                    h[h_rows(e), pl.ds(col, width)] = value

                for b in range(n_blocks):
                    swiglu_block(lambda: xg[x_rows, :], w1, wbuf.at[slot, 1], b, store_h)

            @pl.when(exp == RING)
            def _():
                with jax.named_scope('early_wait'):
                    for b in range(n_blocks):
                        early_block(b).wait()
                        wait(expert_block(exp, b, (1,)))
                with jax.named_scope('early'):
                    whole(RING, (RING + 2) % RING, h.at[early_rows])
                    for b in range(n_blocks):
                        start(expert_block(exp + RING, b, (1,)))

            @pl.when(exp != RING)
            def _():
                with jax.named_scope('w_wait'):
                    for b in range(n_blocks):
                        wait(expert_block(exp, b))
                with jax.named_scope('expert'):
                    whole(exp, place, wbuf.at[place, 0])

                    @pl.when(exp == 0)
                    def _():
                        for b in range(n_blocks):
                            start(expert_block(exp + RING, b, (1,)))
                        for b in range(n_blocks):
                            start(expert_block(exp + 2 * RING, b, (0,)))

                    @pl.when(exp > 0)
                    def _():
                        for b in range(n_blocks):
                            start_after(exp, b)
            return carry
        lax.fori_loop(0, GROUP, expert_step, 0)
        return carry
    lax.fori_loop(0, n_exp // GROUP, group_step, 0)

    for sub in range(n_ring, n_sub):
        start_tile(sub)

    def combine(d):
        r = rbuf[d]
        return jnp.dot(gs[d], jnp.concatenate([r, r, r], axis=0), preferred_element_type=F32)

    def to_partner3(j):
        return remote(send3, recv3.at[lax.rem(j, 4)], s3_send, r3_sem.at[j], partner)

    def to_partner1(j):
        return remote(send1, recv1.at[lax.rem(j, 4)], s1_send, r1_sem.at[j], partner)

    def to_across(j):
        return remote(recv3.at[lax.rem(j, 4)], recvu.at[lax.rem(j, 6)], su_send.at[j], ru_sem.at[j], across)

    def finish(j):
        to_partner1(j).wait_recv()
        to_across(j).wait_recv()
        col = pl.ds(pl.multiple_of(j * CHUNK, CHUNK), CHUNK)
        y[:, col] = (acc[j] + recv1[lax.rem(j, 4)] + recvu[lax.rem(j, 6)]).astype(y.dtype)

    def chunk_step(j, first):
        for begin in range(0, n_exp, BATCH):
            batch = range(begin, begin + BATCH)
            with jax.named_scope('t_wait'):
                for exp in batch:
                    tile_copy(first + exp, j).wait()
            with jax.named_scope('tiles'):
                for exp in batch:
                    r = jnp.dot(h[pl.ds(exp * rows, rows), :], tile_place(first + exp)[...], preferred_element_type=F32).astype(BF16)
                    for d in range(4):
                        rbuf[d, pl.ds(exp * cap, cap), :] = r[d * cap:(d + 1) * cap]

            @pl.when(j + 2 < n_chunks)
            def _():
                for exp in batch:
                    tile_copy(first + exp, j + 2).start()

        @pl.when(j >= 3)
        def _():
            with jax.named_scope('su_wait'):
                to_across(j - 3).wait_send()

        @pl.when(j >= 1)
        def _():
            to_partner3(j - 1).wait_send()
            to_partner1(j - 1).wait_send()

        with jax.named_scope('combine3'):
            send3[...] = combine(3)
            to_partner3(j).start()
        with jax.named_scope('combine210'):
            part2 = combine(2)
            send1[...] = combine(1)
            acc[j] = acc[j] + combine(0)
            to_partner1(j).start()
        with jax.named_scope('pwait'):
            to_partner3(j).wait_recv()
            recv3[lax.rem(j, 4)] = recv3[lax.rem(j, 4)] + part2
            to_across(j).start()

        @pl.when(j >= LAG)
        def _():
            with jax.named_scope('finish'):
                finish(j - LAG)

    def two_chunks(i, carry):
        chunk_step(2 * i, 0)
        chunk_step(2 * i + 1, n_exp)
        return carry
    lax.fori_loop(0, n_chunks // 2, two_chunks, 0)

    def last_step(j, carry):
        with jax.named_scope('last'):
            finish(j)
        return carry
    lax.fori_loop(n_chunks - LAG, n_chunks, last_step, 0)

    for copy in rt_copies + tok_across + tok_relay + [tok_partner]:
        copy.wait_send()
    to_partner3(n_chunks - 1).wait_send()
    to_partner1(n_chunks - 1).wait_send()
    for j in range(n_chunks - 3, n_chunks):
        to_across(j).wait_send()


def solution(mesh):
    num_ep = mesh.shape['ep']
    row_spec = P(('dp', 'ep'), None)
    expert_spec = P('ep', None, None)

    def device_step(tokens, expert_ids, gate_vals, slots, shared_w1, shared_w3, shared_w2, shared_gate, expert_w1, expert_w3, expert_w2):
        n_tok, hidden = tokens.shape
        top_k = expert_ids.shape[1]
        n_exp, _, ff = expert_w1.shape
        num_experts = n_exp * num_ep
        cap = 8 * ((2 * n_tok * top_k + 8 * num_experts - 1) // (8 * num_experts))
        rows = num_ep * cap
        n_chunks = hidden // CHUNK
        n_sub = 2 * n_exp
        n_tail = n_sub - RING * 2 * (ff // CHUNK)
        n_blocks = -(-ff // BLOCK)

        anywhere = pl.BlockSpec(memory_space=pl.ANY)
        dma = pltpu.SemaphoreType.DMA
        vm = pltpu.VMEM
        block = (n_tok, CHUNK)
        return pl.pallas_call(
            functools.partial(moe_kernel, (n_tok, hidden, n_exp, ff, cap, top_k)),
            out_shape=pltpu.VMEM((n_tok, hidden), tokens.dtype),
            in_specs=[anywhere] * 11,
            out_specs=pl.BlockSpec(memory_space=pltpu.VMEM),
            scratch_shapes=[
                vm((4, n_tok, hidden), BF16),
                vm((top_k, n_tok), jnp.int32), vm((top_k, n_tok), jnp.int32), vm((top_k, n_tok), F32),
                vm((hidden // 128, 128), BF16),
                vm((4, 16, n_tok), F32),
                vm((RING, 2, hidden, ff), BF16),
                vm((n_tail, ff, CHUNK), BF16),
                vm((GROUP * rows, hidden), BF16),
                vm((n_exp * rows, ff), BF16),
                vm((4, n_tok, 3 * n_exp * cap), BF16),
                vm((4, n_exp * cap, CHUNK), BF16),
                vm((n_tok, 128), F32),
                vm((n_chunks,) + block, F32),
                vm(block, F32), vm(block, F32),
                vm((4,) + block, F32), vm((4,) + block, F32), vm((6,) + block, F32),
                dma((5,)), dma((RING, 2, n_blocks)), dma((n_blocks,)), dma((n_sub,)),
                dma((2 * PIECES + 1,)), dma((2 * PIECES + 1,)), dma((4,)), dma((4,)),
                dma, dma, dma((n_chunks,)),
                dma((n_chunks,)), dma((n_chunks,)), dma((n_chunks,)),
            ],
            compiler_params=pltpu.CompilerParams(collective_id=0, has_side_effects=True, vmem_limit_bytes=65994752),
        )(tokens, expert_ids.T, slots.T, gate_vals.T, shared_gate.reshape(hidden // 128, 128),
          shared_w1, shared_w3, shared_w2, expert_w1, expert_w3, expert_w2)

    return jax.shard_map(device_step, mesh=mesh, in_specs=(row_spec, row_spec, row_spec, row_spec, P(), P(), P(), P(), expert_spec, expert_spec, expert_spec), out_specs=row_spec, check_vma=False)
```

```python
import functools

import jax
import jax.numpy as jnp
from jax import lax
from jax.experimental import pallas as pl
from jax.experimental.pallas import tpu as pltpu
from jax.sharding import PartitionSpec as P

MESH = pl.DeviceIdType.MESH
F32 = jnp.float32
BF16 = jnp.bfloat16
CHUNK = 256
BLOCK = 512
RING = 3
PIECES = 8
GROUP = 4
BATCH = 8
LAG = 2
BF16_MAX = 3.3895313892515355e38


def moe_kernel(cfg, tok, ids, slots, gates, sgate, sw1, sw3, sw2, ew1, ew3, ew2, y,
               toks, ids_v, slots_v, gates_v, sgate_v, rts, wbuf, wtail, xg, h, gs, rbuf, sig, acc,
               send3, send1, recv3, recv1, recvu,
               load_sem, wsem, early_sem, tsem, tok_send, tok_recv, rt_send, rt_recv,
               s3_send, s1_send, su_send, r3_sem, r1_sem, ru_sem):
    n_tok, hidden, n_exp, ff, cap, top_k = cfg
    rows = 4 * cap
    n_chunks = hidden // CHUNK
    offsets = list(range(0, ff, BLOCK))
    widths = [min(BLOCK, ff - o) for o in offsets]
    n_blocks = len(offsets)
    per_place = 2 * (ff // CHUNK)
    n_ring = RING * per_place
    n_sub = 2 * n_exp
    piece = n_tok // PIECES
    slots_all = n_exp * cap

    dp = lax.axis_index('dp')
    me = lax.axis_index('ep')
    partner = (dp, me + 1 - 2 * lax.rem(me, 2))
    across = (dp, lax.rem(me + 2, 4))
    diagonal = (dp, 3 - me)

    def block_copies(n, srcs, b, which):
        place = n % RING if isinstance(n, int) else lax.rem(n, RING)
        col = pl.ds(offsets[b], widths[b])
        return [pltpu.make_async_copy(srcs[i], wbuf.at[place, i, :, col], wsem.at[place, i, b]) for i in which]

    def shared_block(half, b):
        col = pl.ds(half * ff + offsets[b], widths[b])
        return block_copies(half, (sw1.at[:, col], sw3.at[:, col]), b, (0, 1))

    def expert_block(exp, b, which=(0, 1)):
        col = pl.ds(offsets[b], widths[b])
        return block_copies(exp + 2, (ew1.at[exp, :, col], ew3.at[exp, :, col]), b, which)

    def start(copies):
        for copy in copies:
            copy.start()

    def wait(copies):
        for copy in copies:
            copy.wait()

    def tiles_in(b):
        return range(offsets[b] // CHUNK * 2, (offsets[b] + widths[b]) // CHUNK * 2)

    def start_after(exp, b):
        @pl.when(exp + RING < n_exp)
        def _():
            start(expert_block(exp + RING, b))

        for later in range(RING - 1):
            @pl.when(exp == n_exp - RING + later)
            def _():
                for t in tiles_in(b):
                    start_tile(later * per_place + t)

    early_rows = pl.ds(n_exp * rows - hidden, hidden)

    def early_block(b):
        col = pl.ds(offsets[b], widths[b])
        return pltpu.make_async_copy(ew1.at[RING, :, col], h.at[early_rows, col], early_sem.at[b])

    def tile_place(sub):
        if sub >= n_ring:
            return wtail.at[sub - n_ring]
        place, r = divmod(sub, per_place)
        return wbuf.at[(n_exp + 2 + place) % RING, r % 2, pl.ds(0, ff), pl.ds(r // 2 * CHUNK, CHUNK)]

    def tile_copy(sub, chunk):
        col = pl.ds(pl.multiple_of(chunk * CHUNK, CHUNK), CHUNK)
        return pltpu.make_async_copy(ew2.at[sub % n_exp, :, col], tile_place(sub), tsem.at[sub])

    def start_tile(sub):
        tile_copy(sub, sub // n_exp).start()

    n_held = (n_exp * rows // ff) * (ff // CHUNK)

    def shared_place(tile):
        if tile < n_held:
            row, lane = divmod(tile, ff // CHUNK)
            return h.at[pl.ds(row * ff, ff), pl.ds(lane * CHUNK, CHUNK)]
        lane, which = divmod(tile - n_held, 2)
        return wbuf.at[0, which, pl.ds(0, ff), pl.ds(lane * CHUNK, CHUNK)]

    def shared_tile(tile):
        chunk, half = divmod(tile, 2)
        return pltpu.make_async_copy(sw2.at[pl.ds(half * ff, ff), pl.ds(chunk * CHUNK, CHUNK)],
                                     shared_place(tile), tsem.at[tile])

    def remote(src, dst, send, recv, peer):
        return pltpu.make_async_remote_copy(src_ref=src, dst_ref=dst, send_sem=send, recv_sem=recv,
                                            device_id=peer, device_id_type=MESH)

    def piece_of(ref, i):
        return ref.at[pl.ds(i * piece, piece)]

    barrier = pltpu.get_barrier_semaphore()
    for peer in (partner, across, diagonal):
        pl.semaphore_signal(barrier, inc=1, device_id=peer, device_id_type=MESH)
    tok_loads = [pltpu.make_async_copy(piece_of(tok, i), piece_of(toks.at[0], i), load_sem.at[i]) for i in range(PIECES)]
    loads = [pltpu.make_async_copy(src, dst, load_sem.at[PIECES + i]) for i, (src, dst) in enumerate(
        ((ids, ids_v), (slots, slots_v), (gates, gates_v), (sgate, sgate_v)))]
    start(loads + tok_loads)
    start(shared_block(0, 0))
    with jax.named_scope('own_load'):
        wait(loads)
    dest = jnp.where(slots_v[...] >= 0, ids_v[...] * cap + slots_v[...], -1).astype(F32)
    rts[0] = jnp.zeros_like(rts[0])
    rts[0, 0:top_k, :] = dest
    rts[0, 8:8 + top_k, :] = gates_v[...]
    with jax.named_scope('barrier'):
        pl.semaphore_wait(barrier, 3)

    tok_across = [remote(piece_of(toks.at[0], i), piece_of(toks.at[2], i), tok_send.at[i], tok_recv.at[i], across)
                  for i in range(PIECES)]
    tok_partner = remote(toks.at[0], toks.at[1], tok_send.at[2 * PIECES], tok_recv.at[2 * PIECES], partner)
    rt_copies = [remote(rts.at[0], rts.at[d], rt_send.at[d], rt_recv.at[d], peer)
                 for d, peer in ((1, partner), (2, across), (3, diagonal))]
    start(rt_copies)
    for load, copy in zip(tok_loads, tok_across):
        load.wait()
        copy.start()
    tok_partner.start()
    for half in range(2):
        for b in range(n_blocks):
            if (half, b) != (0, 0):
                start(shared_block(half, b))
    for tile in range(n_held):
        shared_tile(tile).start()
    for b in range(n_blocks):
        start(expert_block(0, b))
    tok_relay = [remote(piece_of(toks.at[2], i), piece_of(toks.at[3], i), tok_send.at[PIECES + i],
                        tok_recv.at[PIECES + i], partner) for i in range(PIECES)]

    def relay(begin, end):
        for i in range(begin, end):
            tok_across[i].wait_recv()
            tok_relay[i].start()

    def swiglu_block(x, w1, w3, b, store):
        done = 0
        while done < widths[b]:
            width = min(CHUNK, widths[b] - done)
            if width == CHUNK:
                a = jnp.dot(x(), w1[:, pl.ds(offsets[b] + done, width)], preferred_element_type=F32)
                g = jnp.dot(x(), w3[:, pl.ds(offsets[b] + done, width)], preferred_element_type=F32)
            else:
                w = jnp.concatenate([w1[:, pl.ds(offsets[b] + done, width)], w3[:, pl.ds(offsets[b] + done, width)]], axis=1)
                both = jnp.dot(x(), w, preferred_element_type=F32)
                a, g = both[:, :width], both[:, width:]
            store(offsets[b] + done, width, (jax.nn.silu(a) * g).astype(BF16))
            done += width

    with jax.named_scope('shared'):
        for half in range(2):
            for b in range(n_blocks):
                wait(shared_block(half, b))

                def store_shared(col, width, value):
                    xg[pl.ds(half * n_tok, n_tok), pl.ds(col, width)] = value

                swiglu_block(lambda: toks[0], wbuf.at[half, 0], wbuf.at[half, 1], b, store_shared)
                if half == 0:
                    for t in tiles_in(b):
                        if n_held + t < 2 * n_chunks:
                            shared_tile(n_held + t).start()

    total = jnp.zeros((n_tok, 128), F32)
    for i in range(hidden // 128):
        total += toks[0, :, pl.ds(i * 128, 128)].astype(F32) * sgate_v[i:i + 1, :].astype(F32)
    logit = jnp.sum(total, axis=1, keepdims=True)
    sig[...] = jnp.broadcast_to(jax.nn.sigmoid(logit), sig.shape)

    with jax.named_scope('shared2'):
        for b in range(n_blocks):
            start(expert_block(2, b))
        for chunk in range(n_chunks):
            for half in range(2):
                shared_tile(2 * chunk + half).wait()
            s = sum(jnp.dot(xg[pl.ds(half * n_tok, n_tok), pl.ds(0, ff)], shared_place(2 * chunk + half)[...],
                            preferred_element_type=F32) for half in range(2))
            acc[chunk] = toks[0, :, pl.ds(chunk * CHUNK, CHUNK)].astype(F32) + sig[:, 0:1] * s
        for b in range(n_blocks):
            start(expert_block(1, b))
        for b in range(n_blocks):
            early_block(b).start()

    relay(0, PIECES // 2)
    with jax.named_scope('wait_near'):
        for copy in rt_copies:
            copy.wait_recv()
        tok_partner.wait_recv()
    base = (me * slots_all).astype(F32)

    with jax.named_scope('weights'):
        for d in range(4):
            def weight_block(i, carry):
                row = (lax.broadcasted_iota(jnp.int32, (128, n_tok), 0) + i * 128).astype(F32) + base
                g = jnp.zeros((128, n_tok), F32)
                for k in range(top_k):
                    g += jnp.where(row == rts[d, k:k + 1, :], rts[d, 8 + k:9 + k, :], 0.0)
                g = g.T
                g1 = jnp.minimum(g, BF16_MAX).astype(BF16)
                left = g - g1.astype(F32)
                g2 = left.astype(BF16)
                g3 = (left - g2.astype(F32)).astype(BF16)
                for part, value in enumerate((g1, g2, g3)):
                    gs[d, :, pl.ds(pl.multiple_of(part * slots_all + i * 128, 128), 128)] = value
                return carry
            lax.fori_loop(0, slots_all // 128, weight_block, 0)

    def gather(g, sources):
        for d in sources:
            row = (lax.broadcasted_iota(jnp.int32, (GROUP * cap, n_tok), 0) + g * (GROUP * cap)).astype(F32) + base
            pick = jnp.zeros((GROUP * cap, n_tok), F32)
            for k in range(top_k):
                pick += jnp.where(row == rts[d, k:k + 1, :], 1.0, 0.0)
            pick = pick.astype(BF16)
            for i in range(hidden // 512):
                col = pl.ds(i * 512, 512)
                got = jnp.dot(pick, toks[d, :, col], preferred_element_type=F32).astype(BF16)
                for e in range(GROUP):
                    xg[pl.ds(e * rows + d * cap, cap), col] = got[e * cap:(e + 1) * cap]

    with jax.named_scope('gather_near'):
        gather(jnp.int32(0), (0, 1))
    relay(PIECES // 2, PIECES - 2)

    with jax.named_scope('dispatch_wait'):
        relay(PIECES - 2, PIECES)
        gather(jnp.int32(0), (2,))
        for copy in tok_relay:
            copy.wait_recv()

    def h_rows(exp):
        return pl.ds(exp * rows if isinstance(exp, int) else pl.multiple_of(exp * rows, rows), rows)

    def group_step(g, carry):
        with jax.named_scope('gather'):
            @pl.when(g == 0)
            def _():
                gather(g, (3,))

            @pl.when(g > 0)
            def _():
                gather(g, range(4))

        def expert_step(i, carry):
            exp = g * GROUP + i
            place = lax.rem(exp + 2, RING)

            def whole(e, slot, w1):
                x_rows = pl.ds(pl.multiple_of(i * rows, rows), rows)

                def store_h(col, width, value):
                    h[h_rows(e), pl.ds(col, width)] = value

                for b in range(n_blocks):
                    swiglu_block(lambda: xg[x_rows, :], w1, wbuf.at[slot, 1], b, store_h)

            @pl.when(exp == RING)
            def _():
                with jax.named_scope('early_wait'):
                    for b in range(n_blocks):
                        early_block(b).wait()
                        wait(expert_block(exp, b, (1,)))
                with jax.named_scope('early'):
                    whole(RING, (RING + 2) % RING, h.at[early_rows])
                    for b in range(n_blocks):
                        start(expert_block(exp + RING, b, (1,)))

            @pl.when(exp != RING)
            def _():
                with jax.named_scope('w_wait'):
                    for b in range(n_blocks):
                        wait(expert_block(exp, b))
                with jax.named_scope('expert'):
                    whole(exp, place, wbuf.at[place, 0])

                    @pl.when(exp == 0)
                    def _():
                        for b in range(n_blocks):
                            start(expert_block(exp + RING, b, (1,)))
                        for b in range(n_blocks):
                            start(expert_block(exp + 2 * RING, b, (0,)))

                    @pl.when(exp > 0)
                    def _():
                        for b in range(n_blocks):
                            start_after(exp, b)
            return carry
        lax.fori_loop(0, GROUP, expert_step, 0)
        return carry
    lax.fori_loop(0, n_exp // GROUP, group_step, 0)

    def combine(d):
        r = rbuf[d]
        return jnp.dot(gs[d], jnp.concatenate([r, r, r], axis=0), preferred_element_type=F32)

    def to_partner3(j):
        return remote(send3, recv3.at[lax.rem(j, 4)], s3_send, r3_sem.at[j], partner)

    def to_partner1(j):
        return remote(send1, recv1.at[lax.rem(j, 4)], s1_send, r1_sem.at[j], partner)

    def to_across(j):
        return remote(recv3.at[lax.rem(j, 4)], recvu.at[lax.rem(j, 6)], su_send.at[j], ru_sem.at[j], across)

    def finish(j):
        to_partner1(j).wait_recv()
        to_across(j).wait_recv()
        col = pl.ds(pl.multiple_of(j * CHUNK, CHUNK), CHUNK)
        y[:, col] = (acc[j] + recv1[lax.rem(j, 4)] + recvu[lax.rem(j, 6)]).astype(y.dtype)

    def tile_rows(first, experts, sources):
        begin, count = sources[0] * cap, len(sources) * cap
        for exp in experts:
            r = jnp.dot(h[pl.ds(exp * rows + begin, count), :], tile_place(first + exp)[...],
                        preferred_element_type=F32).astype(BF16)
            for i, d in enumerate(sources):
                rbuf[d, pl.ds(exp * cap, cap), :] = r[i * cap:(i + 1) * cap]

    def first_chunk():
        for begin in range(0, n_exp, BATCH):
            for exp in range(begin, begin + BATCH):
                tile_copy(exp, 0).wait()
            with jax.named_scope('far_tiles'):
                tile_rows(0, range(begin, begin + BATCH), (2, 3))
            if begin == 0:
                for sub in range((RING - 1) * per_place, n_sub):
                    start_tile(sub)
        with jax.named_scope('far_combine3'):
            send3[...] = combine(3)
            to_partner3(0).start()
        with jax.named_scope('far_combine2'):
            part2 = combine(2)
        with jax.named_scope('pwait0'):
            to_partner3(0).wait_recv()
            recv3[0] = recv3[0] + part2
            to_across(0).start()
        for exp in range(n_exp):
            tile_copy(exp, 2).start()

    def first_chunk_near():
        for exp in range(n_exp):
            tile_copy(exp, 0).wait()
        to_partner1(n_chunks - 1).wait_send()
        with jax.named_scope('near_tiles'):
            tile_rows(0, range(n_exp), (0, 1))
        with jax.named_scope('near_combine'):
            send1[...] = combine(1)
            acc[0] = acc[0] + combine(0)
            to_partner1(0).start()

    def chunk_step(j, first):
        for begin in range(0, n_exp, BATCH):
            batch = range(begin, begin + BATCH)
            with jax.named_scope('t_wait'):
                for exp in batch:
                    tile_copy(first + exp, j).wait()
            with jax.named_scope('tiles'):
                tile_rows(first, batch, range(4))

            @pl.when((j + 2 < n_chunks) | (first == 0))
            def _():
                for exp in batch:
                    tile_copy(first + exp, lax.rem(j + 2, n_chunks)).start()

        @pl.when(j >= 3)
        def _():
            with jax.named_scope('su_wait'):
                to_across(j - 3).wait_send()

        to_partner3(j - 1).wait_send()

        @pl.when(j >= 2)
        def _():
            to_partner1(j - 1).wait_send()

        with jax.named_scope('combine3'):
            send3[...] = combine(3)
            to_partner3(j).start()
        with jax.named_scope('combine210'):
            part2 = combine(2)
            send1[...] = combine(1)
            acc[j] = acc[j] + combine(0)
            to_partner1(j).start()
        with jax.named_scope('pwait'):
            to_partner3(j).wait_recv()
            recv3[lax.rem(j, 4)] = recv3[lax.rem(j, 4)] + part2
            to_across(j).start()

        @pl.when(j == LAG)
        def _():
            to_across(0).wait_recv()
            acc[0] = acc[0] + recvu[0]

        @pl.when(j > LAG)
        def _():
            with jax.named_scope('finish'):
                finish(j - LAG)

    def two_chunks(i, carry):
        @pl.when(i == 0)
        def _():
            first_chunk()

        @pl.when(i > 0)
        def _():
            chunk_step(2 * i, 0)

        chunk_step(2 * i + 1, n_exp)
        return carry
    lax.fori_loop(0, n_chunks // 2, two_chunks, 0)

    first_chunk_near()
    for copy in rt_copies + tok_across + tok_relay + [tok_partner]:
        copy.wait_send()
    to_partner3(n_chunks - 1).wait_send()
    to_partner1(0).wait_recv()
    y[:, pl.ds(0, CHUNK)] = (acc[0] + recv1[0]).astype(y.dtype)
    to_partner1(0).wait_send()
    to_across(n_chunks - 3).wait_send()
    for j in range(n_chunks - LAG, n_chunks):
        to_across(j).wait_send()
        with jax.named_scope('last'):
            finish(j)


def solution(mesh):
    num_ep = mesh.shape['ep']
    row_spec = P(('dp', 'ep'), None)
    expert_spec = P('ep', None, None)

    def device_step(tokens, expert_ids, gate_vals, slots, shared_w1, shared_w3, shared_w2, shared_gate, expert_w1, expert_w3, expert_w2):
        n_tok, hidden = tokens.shape
        top_k = expert_ids.shape[1]
        n_exp, _, ff = expert_w1.shape
        num_experts = n_exp * num_ep
        cap = 8 * ((2 * n_tok * top_k + 8 * num_experts - 1) // (8 * num_experts))
        rows = num_ep * cap
        n_chunks = hidden // CHUNK
        n_sub = 2 * n_exp
        n_tail = n_sub - RING * 2 * (ff // CHUNK)
        n_blocks = -(-ff // BLOCK)

        anywhere = pl.BlockSpec(memory_space=pl.ANY)
        dma = pltpu.SemaphoreType.DMA
        vm = pltpu.VMEM
        block = (n_tok, CHUNK)
        return pl.pallas_call(
            functools.partial(moe_kernel, (n_tok, hidden, n_exp, ff, cap, top_k)),
            out_shape=pltpu.VMEM((n_tok, hidden), tokens.dtype),
            in_specs=[anywhere] * 11,
            out_specs=pl.BlockSpec(memory_space=pltpu.VMEM),
            scratch_shapes=[
                vm((4, n_tok, hidden), BF16),
                vm((top_k, n_tok), jnp.int32), vm((top_k, n_tok), jnp.int32), vm((top_k, n_tok), F32),
                vm((hidden // 128, 128), BF16),
                vm((4, 16, n_tok), F32),
                vm((RING, 2, hidden, ff), BF16),
                vm((n_tail, ff, CHUNK), BF16),
                vm((GROUP * rows, hidden), BF16),
                vm((n_exp * rows, ff), BF16),
                vm((4, n_tok, 3 * n_exp * cap), BF16),
                vm((4, n_exp * cap, CHUNK), BF16),
                vm((n_tok, 128), F32),
                vm((n_chunks,) + block, F32),
                vm(block, F32), vm(block, F32),
                vm((4,) + block, F32), vm((4,) + block, F32), vm((6,) + block, F32),
                dma((PIECES + 4,)), dma((RING, 2, n_blocks)), dma((n_blocks,)), dma((n_sub,)),
                dma((2 * PIECES + 1,)), dma((2 * PIECES + 1,)), dma((4,)), dma((4,)),
                dma, dma, dma((n_chunks,)),
                dma((n_chunks,)), dma((n_chunks,)), dma((n_chunks,)),
            ],
            compiler_params=pltpu.CompilerParams(collective_id=0, has_side_effects=True, vmem_limit_bytes=65994752),
        )(tokens, expert_ids.T, slots.T, gate_vals.T, shared_gate.reshape(hidden // 128, 128),
          shared_w1, shared_w3, shared_w2, expert_w1, expert_w3, expert_w2)

    return jax.shard_map(device_step, mesh=mesh, in_specs=(row_spec, row_spec, row_spec, row_spec, P(), P(), P(), P(), expert_spec, expert_spec, expert_spec), out_specs=row_spec, check_vma=False)
```

```python
import functools

import jax
import jax.numpy as jnp
from jax import lax
from jax.experimental import pallas as pl
from jax.experimental.pallas import tpu as pltpu
from jax.sharding import PartitionSpec as P

MESH = pl.DeviceIdType.MESH
F32 = jnp.float32
BF16 = jnp.bfloat16
CHUNK = 256
BLOCK = 512
RING = 3
PIECES = 8
GROUP = 4
BATCH = 8
LAG = 2
AHEAD = 1
BF16_MAX = 3.3895313892515355e38


def moe_kernel(cfg, tok, ids, slots, gates, sgate, sw1, sw3, sw2, ew1, ew3, ew2, y,
               toks, ids_v, slots_v, gates_v, sgate_v, rts, wbuf, wtail, xg, h, gs, rbuf, sig, acc,
               send3, send1, recv3, recv1, recvu,
               load_sem, wsem, early_sem, tsem, tok_send, tok_recv, rt_send, rt_recv,
               s3_send, s1_send, su_send, r3_sem, r1_sem, ru_sem):
    n_tok, hidden, n_exp, ff, cap, top_k = cfg
    rows = 4 * cap
    n_chunks = hidden // CHUNK
    offsets = list(range(0, ff, BLOCK))
    widths = [min(BLOCK, ff - o) for o in offsets]
    n_blocks = len(offsets)
    per_place = 2 * (ff // CHUNK)
    n_ring = RING * per_place
    n_sub = 2 * n_exp
    piece = n_tok // PIECES
    slots_all = n_exp * cap

    dp = lax.axis_index('dp')
    me = lax.axis_index('ep')
    partner = (dp, me + 1 - 2 * lax.rem(me, 2))
    across = (dp, lax.rem(me + 2, 4))
    diagonal = (dp, 3 - me)

    def block_copies(n, srcs, b, which):
        place = n % RING if isinstance(n, int) else lax.rem(n, RING)
        col = pl.ds(offsets[b], widths[b])
        return [pltpu.make_async_copy(srcs[i], wbuf.at[place, i, :, col], wsem.at[place, i, b]) for i in which]

    def shared_block(half, b):
        col = pl.ds(half * ff + offsets[b], widths[b])
        return block_copies(half, (sw1.at[:, col], sw3.at[:, col]), b, (0, 1))

    def expert_block(exp, b, which=(0, 1)):
        col = pl.ds(offsets[b], widths[b])
        return block_copies(exp + 2, (ew1.at[exp, :, col], ew3.at[exp, :, col]), b, which)

    def start(copies):
        for copy in copies:
            copy.start()

    def wait(copies):
        for copy in copies:
            copy.wait()

    def tiles_in(b):
        return range(offsets[b] // CHUNK * 2, (offsets[b] + widths[b]) // CHUNK * 2)

    def start_after(exp, b):
        @pl.when(exp + RING < n_exp)
        def _():
            start(expert_block(exp + RING, b))

        for later in range(RING - 1):
            @pl.when(exp == n_exp - RING + later)
            def _():
                for t in tiles_in(b):
                    start_tile(later * per_place + t)

    early_rows = pl.ds(n_exp * rows - hidden, hidden)

    def early_block(b):
        col = pl.ds(offsets[b], widths[b])
        return pltpu.make_async_copy(ew1.at[RING, :, col], h.at[early_rows, col], early_sem.at[b])

    def tile_place(sub):
        if sub >= n_ring:
            return wtail.at[sub - n_ring]
        place, r = divmod(sub, per_place)
        return wbuf.at[(n_exp + 2 + place) % RING, r % 2, pl.ds(0, ff), pl.ds(r // 2 * CHUNK, CHUNK)]

    def tile_copy(sub, chunk):
        col = pl.ds(pl.multiple_of(chunk * CHUNK, CHUNK), CHUNK)
        return pltpu.make_async_copy(ew2.at[sub % n_exp, :, col], tile_place(sub), tsem.at[sub])

    def start_tile(sub):
        tile_copy(sub, sub // n_exp).start()

    n_held = (n_exp * rows // ff) * (ff // CHUNK)

    def shared_place(tile):
        if tile < n_held:
            row, lane = divmod(tile, ff // CHUNK)
            return h.at[pl.ds(row * ff, ff), pl.ds(lane * CHUNK, CHUNK)]
        lane, which = divmod(tile - n_held, 2)
        return wbuf.at[0, which, pl.ds(0, ff), pl.ds(lane * CHUNK, CHUNK)]

    def shared_tile(tile):
        chunk, half = divmod(tile, 2)
        return pltpu.make_async_copy(sw2.at[pl.ds(half * ff, ff), pl.ds(chunk * CHUNK, CHUNK)],
                                     shared_place(tile), tsem.at[tile])

    def remote(src, dst, send, recv, peer):
        return pltpu.make_async_remote_copy(src_ref=src, dst_ref=dst, send_sem=send, recv_sem=recv,
                                            device_id=peer, device_id_type=MESH)

    def piece_of(ref, i):
        return ref.at[pl.ds(i * piece, piece)]

    barrier = pltpu.get_barrier_semaphore()
    for peer in (partner, across, diagonal):
        pl.semaphore_signal(barrier, inc=1, device_id=peer, device_id_type=MESH)
    tok_loads = [pltpu.make_async_copy(piece_of(tok, i), piece_of(toks.at[0], i), load_sem.at[i]) for i in range(PIECES)]
    loads = [pltpu.make_async_copy(src, dst, load_sem.at[PIECES + i]) for i, (src, dst) in enumerate(
        ((ids, ids_v), (slots, slots_v), (gates, gates_v), (sgate, sgate_v)))]
    start(loads + tok_loads)
    start(shared_block(0, 0))
    with jax.named_scope('own_load'):
        wait(loads)
    dest = jnp.where(slots_v[...] >= 0, ids_v[...] * cap + slots_v[...], -1).astype(F32)
    rts[0] = jnp.zeros_like(rts[0])
    rts[0, 0:top_k, :] = dest
    rts[0, 8:8 + top_k, :] = gates_v[...]
    with jax.named_scope('barrier'):
        pl.semaphore_wait(barrier, 3)

    tok_across = [remote(piece_of(toks.at[0], i), piece_of(toks.at[2], i), tok_send.at[i], tok_recv.at[i], across)
                  for i in range(PIECES)]
    tok_partner = remote(toks.at[0], toks.at[1], tok_send.at[2 * PIECES], tok_recv.at[2 * PIECES], partner)
    rt_copies = [remote(rts.at[0], rts.at[d], rt_send.at[d], rt_recv.at[d], peer)
                 for d, peer in ((1, partner), (2, across), (3, diagonal))]
    start(rt_copies)
    for load, copy in zip(tok_loads, tok_across):
        load.wait()
        copy.start()
    tok_partner.start()
    for half in range(2):
        for b in range(n_blocks):
            if (half, b) != (0, 0):
                start(shared_block(half, b))
    for tile in range(n_held):
        shared_tile(tile).start()
    for b in range(n_blocks):
        start(expert_block(0, b))
    tok_relay = [remote(piece_of(toks.at[2], i), piece_of(toks.at[3], i), tok_send.at[PIECES + i],
                        tok_recv.at[PIECES + i], partner) for i in range(PIECES)]

    def relay(begin, end):
        for i in range(begin, end):
            tok_across[i].wait_recv()
            tok_relay[i].start()

    def swiglu_block(x, w1, w3, b, store):
        done = 0
        while done < widths[b]:
            width = min(CHUNK, widths[b] - done)
            if width == CHUNK:
                a = jnp.dot(x(), w1[:, pl.ds(offsets[b] + done, width)], preferred_element_type=F32)
                g = jnp.dot(x(), w3[:, pl.ds(offsets[b] + done, width)], preferred_element_type=F32)
            else:
                w = jnp.concatenate([w1[:, pl.ds(offsets[b] + done, width)], w3[:, pl.ds(offsets[b] + done, width)]], axis=1)
                both = jnp.dot(x(), w, preferred_element_type=F32)
                a, g = both[:, :width], both[:, width:]
            store(offsets[b] + done, width, (jax.nn.silu(a) * g).astype(BF16))
            done += width

    with jax.named_scope('shared'):
        for half in range(2):
            for b in range(n_blocks):
                wait(shared_block(half, b))

                def store_shared(col, width, value):
                    xg[pl.ds(half * n_tok, n_tok), pl.ds(col, width)] = value

                swiglu_block(lambda: toks[0], wbuf.at[half, 0], wbuf.at[half, 1], b, store_shared)
                if half == 0:
                    for t in tiles_in(b):
                        if n_held + t < 2 * n_chunks:
                            shared_tile(n_held + t).start()

    total = jnp.zeros((n_tok, 128), F32)
    for i in range(hidden // 128):
        total += toks[0, :, pl.ds(i * 128, 128)].astype(F32) * sgate_v[i:i + 1, :].astype(F32)
    logit = jnp.sum(total, axis=1, keepdims=True)
    sig[...] = jnp.broadcast_to(jax.nn.sigmoid(logit), sig.shape)

    with jax.named_scope('shared2'):
        for b in range(n_blocks):
            start(expert_block(2, b))
        for chunk in range(n_chunks):
            for half in range(2):
                shared_tile(2 * chunk + half).wait()
            s = sum(jnp.dot(xg[pl.ds(half * n_tok, n_tok), pl.ds(0, ff)], shared_place(2 * chunk + half)[...],
                            preferred_element_type=F32) for half in range(2))
            acc[chunk] = toks[0, :, pl.ds(chunk * CHUNK, CHUNK)].astype(F32) + sig[:, 0:1] * s
        for b in range(n_blocks):
            start(expert_block(1, b))
        for b in range(n_blocks):
            early_block(b).start()

    relay(0, PIECES // 2)
    with jax.named_scope('wait_near'):
        for copy in rt_copies:
            copy.wait_recv()
        tok_partner.wait_recv()
    base = (me * slots_all).astype(F32)

    with jax.named_scope('weights'):
        for d in range(4):
            def weight_block(i):
                row = (lax.broadcasted_iota(jnp.int32, (128, n_tok), 0) + i * 128).astype(F32) + base
                g = jnp.zeros((128, n_tok), F32)
                for k in range(top_k):
                    g += jnp.where(row == rts[d, k:k + 1, :], rts[d, 8 + k:9 + k, :], 0.0)
                g = g.T
                g1 = jnp.minimum(g, BF16_MAX).astype(BF16)
                left = g - g1.astype(F32)
                g2 = left.astype(BF16)
                g3 = (left - g2.astype(F32)).astype(BF16)
                for part, value in enumerate((g1, g2, g3)):
                    gs[d, :, pl.ds(pl.multiple_of(part * slots_all + i * 128, 128), 128)] = value

            def weight_step(i, carry):
                for u in range(3):
                    weight_block(3 * i + u)
                return carry
            lax.fori_loop(0, slots_all // 384, weight_step, 0)

    def gather(g, sources):
        for d in sources:
            row = (lax.broadcasted_iota(jnp.int32, (GROUP * cap, n_tok), 0) + g * (GROUP * cap)).astype(F32) + base
            pick = jnp.zeros((GROUP * cap, n_tok), F32)
            for k in range(top_k):
                pick += jnp.where(row == rts[d, k:k + 1, :], 1.0, 0.0)
            pick = pick.astype(BF16)
            for i in range(hidden // 512):
                col = pl.ds(i * 512, 512)
                got = jnp.dot(pick, toks[d, :, col], preferred_element_type=F32).astype(BF16)
                for e in range(GROUP):
                    xg[pl.ds(e * rows + d * cap, cap), col] = got[e * cap:(e + 1) * cap]

    def expert_rows(exp, slot, w1, begin=0, count=4 * cap):
        x_rows = pl.ds(pl.multiple_of(lax.rem(exp, GROUP) * rows + begin, 16), count)
        h_rows = exp * rows + begin
        h_rows = pl.ds(h_rows if isinstance(exp, int) else pl.multiple_of(h_rows, 16), count)

        def store_h(col, width, value):
            h[h_rows, pl.ds(col, width)] = value

        for b in range(n_blocks):
            swiglu_block(lambda: xg[x_rows, :], w1, wbuf.at[slot, 1], b, store_h)

    with jax.named_scope('gather_near'):
        gather(jnp.int32(0), (0, 1))
    relay(PIECES // 2, PIECES - 2)

    def ahead_step(exp, carry):
        for b in range(n_blocks):
            wait(expert_block(exp, b))
        place = lax.rem(exp + 2, RING)
        with jax.named_scope('ahead'):
            expert_rows(exp, place, wbuf.at[place, 0], 0, rows // 2)
        return carry
    ahead_step(jnp.int32(0), 0)


    with jax.named_scope('dispatch_wait'):
        relay(PIECES - 2, PIECES)
        gather(jnp.int32(0), (2,))
        for copy in tok_relay:
            copy.wait_recv()

    def group_step(g, carry):
        with jax.named_scope('gather'):
            @pl.when(g == 0)
            def _():
                gather(g, (3,))

            @pl.when(g > 0)
            def _():
                gather(g, range(4))

        def expert_step(i, carry):
            exp = g * GROUP + i
            place = lax.rem(exp + 2, RING)

            @pl.when(exp == RING)
            def _():
                with jax.named_scope('early_wait'):
                    for b in range(n_blocks):
                        early_block(b).wait()
                        wait(expert_block(exp, b, (1,)))
                with jax.named_scope('early'):
                    expert_rows(RING, (RING + 2) % RING, h.at[early_rows])
                    for b in range(n_blocks):
                        start(expert_block(exp + RING, b, (1,)))

            @pl.when(exp < AHEAD)
            def _():
                with jax.named_scope('behind'):
                    expert_rows(exp, place, wbuf.at[place, 0], rows // 2, rows // 2)

                    for b in range(n_blocks):
                        start(expert_block(exp + RING, b, (1,)))
                    for b in range(n_blocks):
                        start(expert_block(exp + 2 * RING, b, (0,)))

            @pl.when((exp >= AHEAD) & (exp != RING))
            def _():
                with jax.named_scope('w_wait'):
                    for b in range(n_blocks):
                        wait(expert_block(exp, b))
                with jax.named_scope('expert'):
                    expert_rows(exp, place, wbuf.at[place, 0])
                    for b in range(n_blocks):
                        start_after(exp, b)
            return carry
        lax.fori_loop(0, GROUP, expert_step, 0)
        return carry
    lax.fori_loop(0, n_exp // GROUP, group_step, 0)

    def combine(d):
        r = rbuf[d]
        return jnp.dot(gs[d], jnp.concatenate([r, r, r], axis=0), preferred_element_type=F32)

    def to_partner3(j):
        return remote(send3, recv3.at[lax.rem(j, 4)], s3_send, r3_sem.at[j], partner)

    def to_partner1(j):
        return remote(send1, recv1.at[lax.rem(j, 4)], s1_send, r1_sem.at[j], partner)

    def to_across(j):
        return remote(recv3.at[lax.rem(j, 4)], recvu.at[lax.rem(j, 6)], su_send.at[j], ru_sem.at[j], across)

    def finish(j):
        to_partner1(j).wait_recv()
        to_across(j).wait_recv()
        col = pl.ds(pl.multiple_of(j * CHUNK, CHUNK), CHUNK)
        y[:, col] = (acc[j] + recv1[lax.rem(j, 4)] + recvu[lax.rem(j, 6)]).astype(y.dtype)

    def tile_rows(first, experts, sources):
        begin, count = sources[0] * cap, len(sources) * cap
        for exp in experts:
            r = jnp.dot(h[pl.ds(exp * rows + begin, count), :], tile_place(first + exp)[...],
                        preferred_element_type=F32).astype(BF16)
            for i, d in enumerate(sources):
                rbuf[d, pl.ds(exp * cap, cap), :] = r[i * cap:(i + 1) * cap]

    def first_chunk():
        for begin in range(0, n_exp, BATCH):
            for exp in range(begin, begin + BATCH):
                tile_copy(exp, 0).wait()
            with jax.named_scope('far_tiles'):
                tile_rows(0, range(begin, begin + BATCH), (2, 3))
            if begin == 0:
                for sub in range((RING - 1) * per_place, n_sub):
                    start_tile(sub)
        with jax.named_scope('far_combine3'):
            send3[...] = combine(3)
            to_partner3(0).start()
        with jax.named_scope('far_combine2'):
            part2 = combine(2)
        with jax.named_scope('pwait0'):
            to_partner3(0).wait_recv()
            recv3[0] = recv3[0] + part2
            to_across(0).start()
        for exp in range(n_exp):
            tile_copy(exp, 2).start()

    def first_chunk_near():
        for exp in range(n_exp):
            tile_copy(exp, 0).wait()
        to_partner1(n_chunks - 1).wait_send()
        with jax.named_scope('near_tiles'):
            tile_rows(0, range(n_exp), (0, 1))
        with jax.named_scope('near_combine'):
            send1[...] = combine(1)
            acc[0] = acc[0] + combine(0)
            to_partner1(0).start()

    def chunk_step(j, first):
        for begin in range(0, n_exp, BATCH):
            batch = range(begin, begin + BATCH)
            with jax.named_scope('t_wait'):
                for exp in batch:
                    tile_copy(first + exp, j).wait()
            with jax.named_scope('tiles'):
                tile_rows(first, batch, range(4))

            @pl.when((j + 2 < n_chunks) | (first == 0))
            def _():
                for exp in batch:
                    tile_copy(first + exp, lax.rem(j + 2, n_chunks)).start()

        @pl.when(j >= 3)
        def _():
            with jax.named_scope('su_wait'):
                to_across(j - 3).wait_send()

        to_partner3(j - 1).wait_send()

        @pl.when(j >= 2)
        def _():
            to_partner1(j - 1).wait_send()

        with jax.named_scope('combine3'):
            send3[...] = combine(3)
            to_partner3(j).start()
        with jax.named_scope('combine210'):
            part2 = combine(2)
            send1[...] = combine(1)
            acc[j] = acc[j] + combine(0)
            to_partner1(j).start()
        with jax.named_scope('pwait'):
            to_partner3(j).wait_recv()
            recv3[lax.rem(j, 4)] = recv3[lax.rem(j, 4)] + part2
            to_across(j).start()

        @pl.when(j == LAG)
        def _():
            to_across(0).wait_recv()
            acc[0] = acc[0] + recvu[0]

        @pl.when(j > LAG)
        def _():
            with jax.named_scope('finish'):
                finish(j - LAG)

    def two_chunks(i, carry):
        @pl.when(i == 0)
        def _():
            first_chunk()

        @pl.when(i > 0)
        def _():
            chunk_step(2 * i, 0)

        chunk_step(2 * i + 1, n_exp)
        return carry
    lax.fori_loop(0, n_chunks // 2, two_chunks, 0)

    first_chunk_near()
    for copy in rt_copies + tok_across + tok_relay + [tok_partner]:
        copy.wait_send()
    to_partner3(n_chunks - 1).wait_send()
    to_partner1(0).wait_recv()
    y[:, pl.ds(0, CHUNK)] = (acc[0] + recv1[0]).astype(y.dtype)
    to_partner1(0).wait_send()
    to_across(n_chunks - 3).wait_send()
    for j in range(n_chunks - LAG, n_chunks):
        to_across(j).wait_send()
        with jax.named_scope('last'):
            finish(j)


def solution(mesh):
    num_ep = mesh.shape['ep']
    row_spec = P(('dp', 'ep'), None)
    expert_spec = P('ep', None, None)

    def device_step(tokens, expert_ids, gate_vals, slots, shared_w1, shared_w3, shared_w2, shared_gate, expert_w1, expert_w3, expert_w2):
        n_tok, hidden = tokens.shape
        top_k = expert_ids.shape[1]
        n_exp, _, ff = expert_w1.shape
        num_experts = n_exp * num_ep
        cap = 8 * ((2 * n_tok * top_k + 8 * num_experts - 1) // (8 * num_experts))
        rows = num_ep * cap
        n_chunks = hidden // CHUNK
        n_sub = 2 * n_exp
        n_tail = n_sub - RING * 2 * (ff // CHUNK)
        n_blocks = -(-ff // BLOCK)

        anywhere = pl.BlockSpec(memory_space=pl.ANY)
        dma = pltpu.SemaphoreType.DMA
        vm = pltpu.VMEM
        block = (n_tok, CHUNK)
        return pl.pallas_call(
            functools.partial(moe_kernel, (n_tok, hidden, n_exp, ff, cap, top_k)),
            out_shape=pltpu.VMEM((n_tok, hidden), tokens.dtype),
            in_specs=[anywhere] * 11,
            out_specs=pl.BlockSpec(memory_space=pltpu.VMEM),
            scratch_shapes=[
                vm((4, n_tok, hidden), BF16),
                vm((top_k, n_tok), jnp.int32), vm((top_k, n_tok), jnp.int32), vm((top_k, n_tok), F32),
                vm((hidden // 128, 128), BF16),
                vm((4, 16, n_tok), F32),
                vm((RING, 2, hidden, ff), BF16),
                vm((n_tail, ff, CHUNK), BF16),
                vm((GROUP * rows, hidden), BF16),
                vm((n_exp * rows, ff), BF16),
                vm((4, n_tok, 3 * n_exp * cap), BF16),
                vm((4, n_exp * cap, CHUNK), BF16),
                vm((n_tok, 128), F32),
                vm((n_chunks,) + block, F32),
                vm(block, F32), vm(block, F32),
                vm((4,) + block, F32), vm((4,) + block, F32), vm((6,) + block, F32),
                dma((PIECES + 4,)), dma((RING, 2, n_blocks)), dma((n_blocks,)), dma((n_sub,)),
                dma((2 * PIECES + 1,)), dma((2 * PIECES + 1,)), dma((4,)), dma((4,)),
                dma, dma, dma((n_chunks,)),
                dma((n_chunks,)), dma((n_chunks,)), dma((n_chunks,)),
            ],
            compiler_params=pltpu.CompilerParams(collective_id=0, has_side_effects=True, vmem_limit_bytes=65994752),
        )(tokens, expert_ids.T, slots.T, gate_vals.T, shared_gate.reshape(hidden // 128, 128),
          shared_w1, shared_w3, shared_w2, expert_w1, expert_w3, expert_w2)

    return jax.shard_map(device_step, mesh=mesh, in_specs=(row_spec, row_spec, row_spec, row_spec, P(), P(), P(), P(), expert_spec, expert_spec, expert_spec), out_specs=row_spec, check_vma=False)
```

```python
import functools

import jax
import jax.numpy as jnp
from jax import lax
from jax.experimental import pallas as pl
from jax.experimental.pallas import tpu as pltpu
from jax.sharding import PartitionSpec as P

MESH = pl.DeviceIdType.MESH
F32 = jnp.float32
BF16 = jnp.bfloat16
CHUNK = 256
BLOCK = 512
RING = 3
PIECES = 16
GROUP = 4
BATCH = 8
LAG = 2
AHEAD = 1
BF16_MAX = 3.3895313892515355e38


def moe_kernel(cfg, tok, ids, slots, gates, sgate, sw1, sw3, sw2, ew1, ew3, ew2, y,
               toks, ids_v, slots_v, gates_v, sgate_v, rts, wbuf, wtail, xg, h, gs, rbuf, sig, acc,
               send3, send1, recv3, recv1, recvu,
               load_sem, wsem, early_sem, tsem, tok_send, tok_recv, rt_send, rt_recv,
               s3_send, s1_send, su_send, r3_sem, r1_sem, ru_sem):
    n_tok, hidden, n_exp, ff, cap, top_k = cfg
    rows = 4 * cap
    n_chunks = hidden // CHUNK
    offsets = list(range(0, ff, BLOCK))
    widths = [min(BLOCK, ff - o) for o in offsets]
    n_blocks = len(offsets)
    per_place = 2 * (ff // CHUNK)
    n_ring = RING * per_place
    n_sub = 2 * n_exp
    piece = n_tok // PIECES
    slots_all = n_exp * cap

    dp = lax.axis_index('dp')
    me = lax.axis_index('ep')
    partner = (dp, me + 1 - 2 * lax.rem(me, 2))
    across = (dp, lax.rem(me + 2, 4))
    diagonal = (dp, 3 - me)

    def block_copies(n, srcs, b, which):
        place = n % RING if isinstance(n, int) else lax.rem(n, RING)
        col = pl.ds(offsets[b], widths[b])
        return [pltpu.make_async_copy(srcs[i], wbuf.at[place, i, :, col], wsem.at[place, i, b]) for i in which]

    def shared_block(half, b):
        col = pl.ds(half * ff + offsets[b], widths[b])
        return block_copies(half, (sw1.at[:, col], sw3.at[:, col]), b, (0, 1))

    def expert_block(exp, b, which=(0, 1)):
        col = pl.ds(offsets[b], widths[b])
        return block_copies(exp + 2, (ew1.at[exp, :, col], ew3.at[exp, :, col]), b, which)

    def start(copies):
        for copy in copies:
            copy.start()

    def wait(copies):
        for copy in copies:
            copy.wait()

    def tiles_in(b):
        return range(offsets[b] // CHUNK * 2, (offsets[b] + widths[b]) // CHUNK * 2)

    def start_after(exp, b):
        @pl.when(exp + RING < n_exp)
        def _():
            start(expert_block(exp + RING, b))

        for later in range(RING - 1):
            @pl.when(exp == n_exp - RING + later)
            def _():
                for t in tiles_in(b):
                    start_tile(later * per_place + t)

    early_rows = pl.ds(n_exp * rows - hidden, hidden)

    def early_block(b):
        col = pl.ds(offsets[b], widths[b])
        return pltpu.make_async_copy(ew1.at[RING, :, col], h.at[early_rows, col], early_sem.at[b])

    def tile_place(sub):
        if sub >= n_ring:
            return wtail.at[sub - n_ring]
        place, r = divmod(sub, per_place)
        return wbuf.at[(n_exp + 2 + place) % RING, r % 2, pl.ds(0, ff), pl.ds(r // 2 * CHUNK, CHUNK)]

    def tile_copy(sub, chunk):
        col = pl.ds(pl.multiple_of(chunk * CHUNK, CHUNK), CHUNK)
        return pltpu.make_async_copy(ew2.at[sub % n_exp, :, col], tile_place(sub), tsem.at[sub])

    def start_tile(sub):
        tile_copy(sub, sub // n_exp).start()

    n_held = (n_exp * rows // ff) * (ff // CHUNK)

    def shared_place(tile):
        if tile < n_held:
            row, lane = divmod(tile, ff // CHUNK)
            return h.at[pl.ds(row * ff, ff), pl.ds(lane * CHUNK, CHUNK)]
        lane, which = divmod(tile - n_held, 2)
        return wbuf.at[0, which, pl.ds(0, ff), pl.ds(lane * CHUNK, CHUNK)]

    def shared_tile(tile):
        chunk, half = divmod(tile, 2)
        return pltpu.make_async_copy(sw2.at[pl.ds(half * ff, ff), pl.ds(chunk * CHUNK, CHUNK)],
                                     shared_place(tile), tsem.at[tile])

    def remote(src, dst, send, recv, peer):
        return pltpu.make_async_remote_copy(src_ref=src, dst_ref=dst, send_sem=send, recv_sem=recv,
                                            device_id=peer, device_id_type=MESH)

    def piece_of(ref, i):
        return ref.at[pl.ds(i * piece, piece)]

    barrier = pltpu.get_barrier_semaphore()
    for peer in (partner, across, diagonal):
        pl.semaphore_signal(barrier, inc=1, device_id=peer, device_id_type=MESH)
    tok_loads = [pltpu.make_async_copy(piece_of(tok, i), piece_of(toks.at[0], i), load_sem.at[i]) for i in range(PIECES)]
    loads = [pltpu.make_async_copy(src, dst, load_sem.at[PIECES + i]) for i, (src, dst) in enumerate(
        ((ids, ids_v), (slots, slots_v), (gates, gates_v), (sgate, sgate_v)))]
    start(loads + tok_loads)
    start(shared_block(0, 0))
    with jax.named_scope('own_load'):
        wait(loads)
    dest = jnp.where(slots_v[...] >= 0, ids_v[...] * cap + slots_v[...], -1).astype(F32)
    rts[0] = jnp.zeros_like(rts[0])
    rts[0, 0:top_k, :] = dest
    rts[0, 8:8 + top_k, :] = gates_v[...]
    with jax.named_scope('barrier'):
        pl.semaphore_wait(barrier, 3)

    tok_across = [remote(piece_of(toks.at[0], i), piece_of(toks.at[2], i), tok_send.at[i], tok_recv.at[i], across)
                  for i in range(PIECES)]
    tok_partner = remote(toks.at[0], toks.at[1], tok_send.at[2 * PIECES], tok_recv.at[2 * PIECES], partner)
    rt_copies = [remote(rts.at[0], rts.at[d], rt_send.at[d], rt_recv.at[d], peer)
                 for d, peer in ((1, partner), (2, across), (3, diagonal))]
    start(rt_copies)
    for load, copy in zip(tok_loads, tok_across):
        load.wait()
        copy.start()
    tok_partner.start()
    for half in range(2):
        for b in range(n_blocks):
            if (half, b) != (0, 0):
                start(shared_block(half, b))
    for tile in range(n_held):
        shared_tile(tile).start()
    for b in range(n_blocks):
        start(expert_block(0, b))
    tok_relay = [remote(piece_of(toks.at[2], i), piece_of(toks.at[3], i), tok_send.at[PIECES + i],
                        tok_recv.at[PIECES + i], partner) for i in range(PIECES)]

    def relay(begin, end):
        for i in range(begin, end):
            tok_across[i].wait_recv()
            tok_relay[i].start()

    def swiglu_block(x, w1, w3, b, store):
        done = 0
        while done < widths[b]:
            width = min(CHUNK, widths[b] - done)
            if width == CHUNK:
                a = jnp.dot(x(), w1[:, pl.ds(offsets[b] + done, width)], preferred_element_type=F32)
                g = jnp.dot(x(), w3[:, pl.ds(offsets[b] + done, width)], preferred_element_type=F32)
            else:
                w = jnp.concatenate([w1[:, pl.ds(offsets[b] + done, width)], w3[:, pl.ds(offsets[b] + done, width)]], axis=1)
                both = jnp.dot(x(), w, preferred_element_type=F32)
                a, g = both[:, :width], both[:, width:]
            store(offsets[b] + done, width, (jax.nn.silu(a) * g).astype(BF16))
            done += width

    with jax.named_scope('shared'):
        for half in range(2):
            for b in range(n_blocks):
                wait(shared_block(half, b))

                def store_shared(col, width, value):
                    xg[pl.ds(half * n_tok, n_tok), pl.ds(col, width)] = value

                swiglu_block(lambda: toks[0], wbuf.at[half, 0], wbuf.at[half, 1], b, store_shared)
                if half == 0:
                    for t in tiles_in(b):
                        if n_held + t < 2 * n_chunks:
                            shared_tile(n_held + t).start()

    total = jnp.zeros((n_tok, 128), F32)
    for i in range(hidden // 128):
        total += toks[0, :, pl.ds(i * 128, 128)].astype(F32) * sgate_v[i:i + 1, :].astype(F32)
    logit = jnp.sum(total, axis=1, keepdims=True)
    sig[...] = jnp.broadcast_to(jax.nn.sigmoid(logit), sig.shape)

    with jax.named_scope('shared2'):
        for b in range(n_blocks):
            start(expert_block(2, b))
        for chunk in range(n_chunks):
            for half in range(2):
                shared_tile(2 * chunk + half).wait()
            s = sum(jnp.dot(xg[pl.ds(half * n_tok, n_tok), pl.ds(0, ff)], shared_place(2 * chunk + half)[...],
                            preferred_element_type=F32) for half in range(2))
            acc[chunk] = toks[0, :, pl.ds(chunk * CHUNK, CHUNK)].astype(F32) + sig[:, 0:1] * s
        for b in range(n_blocks):
            start(expert_block(1, b))
        for b in range(n_blocks):
            early_block(b).start()

    relay(0, PIECES // 2)
    with jax.named_scope('wait_near'):
        for copy in rt_copies:
            copy.wait_recv()
        tok_partner.wait_recv()
    base = (me * slots_all).astype(F32)

    with jax.named_scope('weights'):
        for d in range(4):
            def weight_block(i):
                row = (lax.broadcasted_iota(jnp.int32, (128, n_tok), 0) + i * 128).astype(F32) + base
                g = jnp.zeros((128, n_tok), F32)
                for k in range(top_k):
                    g += jnp.where(row == rts[d, k:k + 1, :], rts[d, 8 + k:9 + k, :], 0.0)
                g = g.T
                g1 = jnp.minimum(g, BF16_MAX).astype(BF16)
                left = g - g1.astype(F32)
                g2 = left.astype(BF16)
                g3 = (left - g2.astype(F32)).astype(BF16)
                for part, value in enumerate((g1, g2, g3)):
                    gs[d, :, pl.ds(pl.multiple_of(part * slots_all + i * 128, 128), 128)] = value

            def weight_step(i, carry):
                for u in range(3):
                    weight_block(3 * i + u)
                return carry
            lax.fori_loop(0, slots_all // 384, weight_step, 0)

    def gather(g, sources):
        for d in sources:
            row = (lax.broadcasted_iota(jnp.int32, (GROUP * cap, n_tok), 0) + g * (GROUP * cap)).astype(F32) + base
            pick = jnp.zeros((GROUP * cap, n_tok), F32)
            for k in range(top_k):
                pick += jnp.where(row == rts[d, k:k + 1, :], 1.0, 0.0)
            pick = pick.astype(BF16)
            for i in range(hidden // 512):
                col = pl.ds(i * 512, 512)
                got = jnp.dot(pick, toks[d, :, col], preferred_element_type=F32).astype(BF16)
                for e in range(GROUP):
                    xg[pl.ds(e * rows + d * cap, cap), col] = got[e * cap:(e + 1) * cap]

    def expert_rows(exp, slot, w1, begin=0, count=4 * cap):
        x_rows = pl.ds(pl.multiple_of(lax.rem(exp, GROUP) * rows + begin, 16), count)
        h_rows = exp * rows + begin
        h_rows = pl.ds(h_rows if isinstance(exp, int) else pl.multiple_of(h_rows, 16), count)

        def store_h(col, width, value):
            h[h_rows, pl.ds(col, width)] = value

        for b in range(n_blocks):
            swiglu_block(lambda: xg[x_rows, :], w1, wbuf.at[slot, 1], b, store_h)

    with jax.named_scope('gather_near'):
        gather(jnp.int32(0), (0, 1))
    relay(PIECES // 2, PIECES - 4)

    def ahead_step(exp, carry):
        for b in range(n_blocks):
            wait(expert_block(exp, b))
        place = lax.rem(exp + 2, RING)
        with jax.named_scope('ahead'):
            expert_rows(exp, place, wbuf.at[place, 0], 0, rows // 2)
        return carry
    ahead_step(jnp.int32(0), 0)


    with jax.named_scope('dispatch_wait'):
        relay(PIECES - 4, PIECES)
        gather(jnp.int32(0), (2,))
        for copy in tok_relay:
            copy.wait_recv()

    def group_step(g, carry):
        with jax.named_scope('gather'):
            @pl.when(g == 0)
            def _():
                gather(g, (3,))

            @pl.when(g > 0)
            def _():
                gather(g, range(4))

        def expert_step(i, carry):
            exp = g * GROUP + i
            place = lax.rem(exp + 2, RING)

            @pl.when(exp == RING)
            def _():
                with jax.named_scope('early_wait'):
                    for b in range(n_blocks):
                        early_block(b).wait()
                        wait(expert_block(exp, b, (1,)))
                with jax.named_scope('early'):
                    expert_rows(RING, (RING + 2) % RING, h.at[early_rows])
                    for b in range(n_blocks):
                        start(expert_block(exp + RING, b, (1,)))

            @pl.when(exp < AHEAD)
            def _():
                with jax.named_scope('behind'):
                    expert_rows(exp, place, wbuf.at[place, 0], rows // 2, rows // 2)

                    for b in range(n_blocks):
                        start(expert_block(exp + RING, b, (1,)))
                    for b in range(n_blocks):
                        start(expert_block(exp + 2 * RING, b, (0,)))

            @pl.when((exp >= AHEAD) & (exp != RING))
            def _():
                with jax.named_scope('w_wait'):
                    for b in range(n_blocks):
                        wait(expert_block(exp, b))
                with jax.named_scope('expert'):
                    expert_rows(exp, place, wbuf.at[place, 0])
                    for b in range(n_blocks):
                        start_after(exp, b)
            return carry
        lax.fori_loop(0, GROUP, expert_step, 0)
        return carry
    lax.fori_loop(0, n_exp // GROUP, group_step, 0)

    def combine(d):
        r = rbuf[d]
        return jnp.dot(gs[d], jnp.concatenate([r, r, r], axis=0), preferred_element_type=F32)

    def to_partner3(j):
        return remote(send3, recv3.at[lax.rem(j, 4)], s3_send, r3_sem.at[j], partner)

    def to_partner1(j):
        return remote(send1, recv1.at[lax.rem(j, 4)], s1_send, r1_sem.at[j], partner)

    def to_across(j):
        return remote(recv3.at[lax.rem(j, 4)], recvu.at[lax.rem(j, 6)], su_send.at[j], ru_sem.at[j], across)

    def finish(j):
        to_partner1(j).wait_recv()
        to_across(j).wait_recv()
        col = pl.ds(pl.multiple_of(j * CHUNK, CHUNK), CHUNK)
        y[:, col] = (acc[j] + recv1[lax.rem(j, 4)] + recvu[lax.rem(j, 6)]).astype(y.dtype)

    def tile_rows(first, experts, sources):
        begin, count = sources[0] * cap, len(sources) * cap
        for exp in experts:
            r = jnp.dot(h[pl.ds(exp * rows + begin, count), :], tile_place(first + exp)[...],
                        preferred_element_type=F32).astype(BF16)
            for i, d in enumerate(sources):
                rbuf[d, pl.ds(exp * cap, cap), :] = r[i * cap:(i + 1) * cap]

    def first_chunk():
        for begin in range(0, n_exp, BATCH):
            for exp in range(begin, begin + BATCH):
                tile_copy(exp, 0).wait()
            with jax.named_scope('far_tiles'):
                tile_rows(0, range(begin, begin + BATCH), (2, 3))
            if begin == 0:
                for sub in range((RING - 1) * per_place, n_sub):
                    start_tile(sub)
        with jax.named_scope('far_combine3'):
            send3[...] = combine(3)
            to_partner3(0).start()
        with jax.named_scope('far_combine2'):
            part2 = combine(2)
        with jax.named_scope('pwait0'):
            to_partner3(0).wait_recv()
            recv3[0] = recv3[0] + part2
            to_across(0).start()
        for exp in range(n_exp):
            tile_copy(exp, 2).start()

    def first_chunk_near():
        for exp in range(n_exp):
            tile_copy(exp, 0).wait()
        to_partner1(n_chunks - 1).wait_send()
        with jax.named_scope('near_tiles'):
            tile_rows(0, range(n_exp), (0, 1))
        with jax.named_scope('near_combine'):
            send1[...] = combine(1)
            acc[0] = acc[0] + combine(0)
            to_partner1(0).start()

    def chunk_step(j, first):
        for begin in range(0, n_exp, BATCH):
            batch = range(begin, begin + BATCH)
            with jax.named_scope('t_wait'):
                for exp in batch:
                    tile_copy(first + exp, j).wait()
            with jax.named_scope('tiles'):
                tile_rows(first, batch, range(4))

            @pl.when((j + 2 < n_chunks) | (first == 0))
            def _():
                for exp in batch:
                    tile_copy(first + exp, lax.rem(j + 2, n_chunks)).start()

        @pl.when(j >= 3)
        def _():
            with jax.named_scope('su_wait'):
                to_across(j - 3).wait_send()

        to_partner3(j - 1).wait_send()

        @pl.when(j >= 2)
        def _():
            to_partner1(j - 1).wait_send()

        with jax.named_scope('combine3'):
            send3[...] = combine(3)
            to_partner3(j).start()
        with jax.named_scope('combine210'):
            part2 = combine(2)
            send1[...] = combine(1)
            acc[j] = acc[j] + combine(0)
            to_partner1(j).start()
        with jax.named_scope('pwait'):
            to_partner3(j).wait_recv()
            recv3[lax.rem(j, 4)] = recv3[lax.rem(j, 4)] + part2
            to_across(j).start()

        @pl.when(j == LAG)
        def _():
            to_across(0).wait_recv()
            acc[0] = acc[0] + recvu[0]

        @pl.when(j > LAG)
        def _():
            with jax.named_scope('finish'):
                finish(j - LAG)

    def two_chunks(i, carry):
        @pl.when(i == 0)
        def _():
            first_chunk()

        @pl.when(i > 0)
        def _():
            chunk_step(2 * i, 0)

        chunk_step(2 * i + 1, n_exp)
        return carry
    lax.fori_loop(0, n_chunks // 2, two_chunks, 0)

    first_chunk_near()
    for copy in rt_copies + tok_across + tok_relay + [tok_partner]:
        copy.wait_send()
    to_partner3(n_chunks - 1).wait_send()
    to_partner1(0).wait_recv()
    y[:, pl.ds(0, CHUNK)] = (acc[0] + recv1[0]).astype(y.dtype)
    to_partner1(0).wait_send()
    to_across(n_chunks - 3).wait_send()
    for j in range(n_chunks - LAG, n_chunks):
        to_across(j).wait_send()
        with jax.named_scope('last'):
            finish(j)


def solution(mesh):
    num_ep = mesh.shape['ep']
    row_spec = P(('dp', 'ep'), None)
    expert_spec = P('ep', None, None)

    def device_step(tokens, expert_ids, gate_vals, slots, shared_w1, shared_w3, shared_w2, shared_gate, expert_w1, expert_w3, expert_w2):
        n_tok, hidden = tokens.shape
        top_k = expert_ids.shape[1]
        n_exp, _, ff = expert_w1.shape
        num_experts = n_exp * num_ep
        cap = 8 * ((2 * n_tok * top_k + 8 * num_experts - 1) // (8 * num_experts))
        rows = num_ep * cap
        n_chunks = hidden // CHUNK
        n_sub = 2 * n_exp
        n_tail = n_sub - RING * 2 * (ff // CHUNK)
        n_blocks = -(-ff // BLOCK)

        anywhere = pl.BlockSpec(memory_space=pl.ANY)
        dma = pltpu.SemaphoreType.DMA
        vm = pltpu.VMEM
        block = (n_tok, CHUNK)
        return pl.pallas_call(
            functools.partial(moe_kernel, (n_tok, hidden, n_exp, ff, cap, top_k)),
            out_shape=pltpu.VMEM((n_tok, hidden), tokens.dtype),
            in_specs=[anywhere] * 11,
            out_specs=pl.BlockSpec(memory_space=pltpu.VMEM),
            scratch_shapes=[
                vm((4, n_tok, hidden), BF16),
                vm((top_k, n_tok), jnp.int32), vm((top_k, n_tok), jnp.int32), vm((top_k, n_tok), F32),
                vm((hidden // 128, 128), BF16),
                vm((4, 16, n_tok), F32),
                vm((RING, 2, hidden, ff), BF16),
                vm((n_tail, ff, CHUNK), BF16),
                vm((GROUP * rows, hidden), BF16),
                vm((n_exp * rows, ff), BF16),
                vm((4, n_tok, 3 * n_exp * cap), BF16),
                vm((4, n_exp * cap, CHUNK), BF16),
                vm((n_tok, 128), F32),
                vm((n_chunks,) + block, F32),
                vm(block, F32), vm(block, F32),
                vm((4,) + block, F32), vm((4,) + block, F32), vm((6,) + block, F32),
                dma((PIECES + 4,)), dma((RING, 2, n_blocks)), dma((n_blocks,)), dma((n_sub,)),
                dma((2 * PIECES + 1,)), dma((2 * PIECES + 1,)), dma((4,)), dma((4,)),
                dma, dma, dma((n_chunks,)),
                dma((n_chunks,)), dma((n_chunks,)), dma((n_chunks,)),
            ],
            compiler_params=pltpu.CompilerParams(collective_id=0, has_side_effects=True, vmem_limit_bytes=65994752),
        )(tokens, expert_ids.T, slots.T, gate_vals.T, shared_gate.reshape(hidden // 128, 128),
          shared_w1, shared_w3, shared_w2, expert_w1, expert_w3, expert_w2)

    return jax.shard_map(device_step, mesh=mesh, in_specs=(row_spec, row_spec, row_spec, row_spec, P(), P(), P(), P(), expert_spec, expert_spec, expert_spec), out_specs=row_spec, check_vma=False)
```
